128 devices in a mesh: zg: 2 (over x_lo), xy: 64 (over x_hi, y, z, core).
Axes of the slice: x: 4 (x_hi: 2, x_lo: 2; x = x_hi * 2 + x_lo), y: 4, z: 4, core: 2. Of those that a mesh axis runs over, the one named last changes fastest.
Arguments:
- charges: float32 [262144], P(('zg', 'xy')), may hold values from -12 to 12
- cells: int32 [8, 262144], P(None, ('zg', 'xy')), may hold values from 0 to 786431
- splines: float32 [8, 262144], P(None, ('zg', 'xy')), may hold values from 0.05 to 1
- counts: int32 [128], P(('zg', 'xy')), may hold values from 1024 to 2048, as said below
- green: bfloat16 [512, 4, 384, 384], P(('zg', 'xy')), may hold values from -0.3125 to 0.3125
Outputs:
- potential: float32 [384, 512, 512], P(('zg', 'xy'))
The draws below stay inside these ranges and needn't reach their ends.
Inputs may be any that keep to these rules, and one draw needn't show every extreme that they name: `counts`: some device has all 2048 slots live in every draw.
All inputs are finite; a program needn't handle non-finite values.
Results may differ from the reference program's by a relative error of at most 0.0041.
Values may be sent and summed in bfloat16 or wider, within the bound.
A program may use at most 64 MiB of HBM per device.

```python
import jax
import jax.numpy as jnp
from jax import lax

NX = 512
NY = 512
NZ = 384
KYB = 4
SPREAD = 8
PART_DEV = 2048
ZDEV = 3
PARTICLES = 262144
N_ZG = 2
N_XY = 64
DEVICES = 128


def draw_counts(key, part):
    first = jax.random.fold_in(key, 11)
    second = jax.random.fold_in(key, 23)
    values = jax.random.randint(first, (DEVICES,), PART_DEV // 2, PART_DEV + 1, dtype=jnp.int32)
    chosen = jax.random.randint(second, (), 0, DEVICES, dtype=jnp.int32)
    places = jnp.arange(DEVICES, dtype=jnp.int32)
    return jnp.where(places == chosen, PART_DEV, values).astype(jnp.int32)


def plant(entries, stream_key, low, top_value):
    index_at = [jax.random.randint(jax.random.fold_in(stream_key, axis), (), 0, length) for axis, length in enumerate(entries.shape)]
    longest = entries.shape.index(max(entries.shape))
    next_to = index_at[:longest] + [(index_at[longest] + 1) % entries.shape[longest]] + index_at[longest + 1:]
    return entries.at[tuple(index_at)].set(low).at[tuple(next_to)].set(top_value)


def steps_of(stream_key, shape, split, smallest, high):
    def one(axis_at, blocks):
        heights = jax.random.uniform(jax.random.fold_in(jax.random.fold_in(stream_key, 6), axis_at), (blocks,), jnp.float32, smallest / len(split), high / len(split))
        return jnp.repeat(jnp.exp(heights), shape[axis_at] // blocks).reshape((-1,) + (1,) * (len(shape) - axis_at - 1))

    level = one(*split[0])
    for cut in split[1:]:
        level = level * one(*cut)
    return level


def normal_values(key, dims, spread, reach, pieces=(), kind=jnp.bfloat16):
    result = spread * jax.random.normal(key, dims, jnp.float32)
    if pieces:
        result = result * steps_of(key, dims, pieces, -0.22, 0.18)
    return jnp.clip(result, -reach, reach).astype(kind)


def setup_inputs(seed: int = 0) -> dict:
    key_list = jax.random.split(jax.random.key(seed), 6)
    charges = normal_values(key_list[0], (PARTICLES,), 2.0, 12.0, ((0, 128),), jnp.float32)
    cells = plant(jax.random.randint(key_list[1], (SPREAD, PARTICLES), 0, ZDEV * NX * NY), jax.random.fold_in(key_list[1], 1), 0, (ZDEV * NX * NY) - 1).astype(jnp.int32)
    splines = jnp.clip(0.05 + 0.95 * jax.random.uniform(key_list[2], (SPREAD, PARTICLES), jnp.float32) ** steps_of(key_list[2], (SPREAD, PARTICLES), ((1, 128),), -0.2, 0.2), 0.05, 1.0)
    counts = draw_counts(jax.random.fold_in(key_list[5], 71), 0)
    green = normal_values(key_list[4], (NX, KYB, NZ, NZ), NZ ** -0.5, 0.3125, ((0, 128),))
    return {"charges": charges, "cells": cells, "splines": splines, "counts": counts, "green": green}


def reference(charges, cells, splines, counts, green):
    devices = N_ZG * N_XY
    slab = NZ // devices
    slots = jnp.arange(devices * PART_DEV, dtype=jnp.int32)
    owner = slots // PART_DEV
    rank = slots - owner * PART_DEV
    live = (rank < counts[owner]).astype(jnp.float32)
    values = splines * (charges * live)[None, :]
    offsets = cells + (owner * (slab * NX * NY))[None, :]
    density = jnp.zeros((NZ * NX * NY,), jnp.float32).at[offsets.reshape(-1)].add(values.reshape(-1))
    density = density.reshape(NZ, NX, NY)
    norm = jnp.sqrt(jnp.float32(NX * NY))
    transformed = jnp.fft.fft2(density, axes=(1, 2)) / norm
    spectrum = jnp.stack([jnp.real(transformed), jnp.imag(transformed)], axis=1).astype(jnp.bfloat16)

    def one_column(pair):
        matrices, plane = pair
        blocks = plane.astype(jnp.float32).reshape(NZ, 2, KYB, NY // KYB)
        mixed = jnp.einsum('bzw,wcbj->zcbj', matrices.astype(jnp.float32), blocks)
        return mixed.reshape(NZ, 2, NY).astype(jnp.bfloat16)
    columns = lax.map(one_column, (green, jnp.moveaxis(spectrum, 2, 0)))
    mixed = jnp.moveaxis(columns, 0, 2).astype(jnp.float32)
    complex_hat = lax.complex(mixed[:, 0], mixed[:, 1])
    potential = jnp.real(jnp.fft.ifft2(complex_hat, axes=(1, 2))) * norm
    return potential.astype(jnp.float32)
```

```python
import functools
import math

import numpy as np
import jax
import jax.numpy as jnp
from jax import lax
from jax.experimental import pallas as pl
from jax.experimental.pallas import tpu as pltpu
from jax.sharding import PartitionSpec as P

NX = 512
NY = 512
NZ = 384
HALF = 256
DEV = 128
SLAB = 3
SLOTS = 2048
SPREAD = 8
CHUNK = 256
CANDIDATES = 32
F32 = jnp.float32
BF16 = jnp.bfloat16


def split_table(table):
    high = table.astype(np.float32).astype(BF16)
    low = (table - high.astype(np.float64)).astype(np.float32).astype(BF16)
    return high, low


def make_tables():
    y = np.arange(NY)[:, None]
    v = np.arange(HALF)[None, :]
    angle = 2.0 * math.pi * (y * v % NY) / NY
    along_p = np.cos(angle)
    along_q = -np.sin(angle)
    along_q[:, 0] = 1.0 - 2.0 * (np.arange(NY) % 2)
    y_high, y_low = split_table(np.concatenate([along_p, along_q], axis=1))
    x = np.arange(HALF)[None, None, :]
    result = [y_high, y_low]
    for parity in range(2):
        u = (4 * np.arange(DEV)[:, None] + 2 * np.arange(2)[None, :] + parity)[:, :, None]
        angle = 2.0 * math.pi * (u * x % NX) / NX
        c, s = np.cos(angle), np.sin(angle)
        rows = [
            np.concatenate([c, s], axis=2),
            np.concatenate([-s, c], axis=2),
            np.concatenate([c, -s], axis=2),
            np.concatenate([-s, -c], axis=2),
        ]
        table = np.stack(rows, axis=1).reshape(DEV * 8, NX)
        result += split_table(table)
    return result


def make_shuffle():
    k, w = np.meshgrid(np.arange(16), np.arange(16), indexing="ij")
    shuffle = np.zeros((256, 256), np.float32)
    shuffle[(k * 16 + w).reshape(-1), (w * 16 + k).reshape(-1)] = 1.0
    return shuffle.astype(BF16)


def dot(a, b):
    return jnp.dot(a, b, preferred_element_type=F32)


def dot_nt(a, b):
    return lax.dot_general(a, b, (((1,), (1,)), ((), ())), preferred_element_type=F32)


def dot_tn(a, b):
    return lax.dot_general(a, b, (((0,), (0,)), ((), ())), preferred_element_type=F32)


def halves(value):
    high = value.astype(BF16)
    return high, (value - high.astype(F32)).astype(BF16)


def factor(value):
    best_left = jnp.ones_like(value)
    best_right = value.astype(BF16).astype(F32)
    best_error = jnp.abs(best_right - value)
    for j in range(1, CANDIDATES):
        left = 1.0 + j * (128 // CANDIDATES) / 128.0
        right = (value * (1.0 / left)).astype(BF16).astype(F32)
        error = jnp.abs(right * left - value)
        better = error < best_error
        best_error = jnp.where(better, error, best_error)
        best_right = jnp.where(better, right, best_right)
        best_left = jnp.where(better, left, best_left)
    return best_left, best_right


def prepare(counts, charges, splines, cells, left_ref, right_ref, row_ref, col_ref):
    slot = lax.broadcasted_iota(jnp.int32, (1, SLOTS), 1)
    live = jnp.where(slot < counts[0], charges[...], 0.0)
    left, right = factor(splines[...] * live)
    left_ref[...] = left
    right_ref[...] = right
    row_ref[...] = lax.shift_right_logical(cells[...], 9)
    col_ref[...] = lax.bitwise_and(cells[...], NY - 1)


def density_of(plane, left_ref, right_ref, row_ref, col_ref, total_ref):
    total_ref[...] = jnp.zeros_like(total_ref)
    index = lax.broadcasted_iota(jnp.int32, (NX, CHUNK), 0)
    index_row = index + plane * NX

    def body(c, carry):
        at = pl.ds(pl.multiple_of(c * CHUNK, CHUNK), CHUNK)
        a, b = [], []
        for k in range(SPREAD):
            a.append(jnp.where(row_ref[k : k + 1, at] == index_row, left_ref[k : k + 1, at], 0.0).astype(BF16))
            b.append(jnp.where(col_ref[k : k + 1, at] == index, right_ref[k : k + 1, at], 0.0).astype(BF16))
        total_ref[...] += dot_nt(jnp.concatenate(a, axis=1), jnp.concatenate(b, axis=1))
        return carry

    lax.fori_loop(0, SLOTS // CHUNK, body, 0)


def plane_spectrum(density, y_high, y_low, x_tables):
    high, low = halves(density)
    along = dot(high, y_high[...]) + dot(high, y_low[...]) + dot(low, y_high[...])
    folds = (along[:HALF] + along[HALF:], along[:HALF] - along[HALF:])
    parts = []
    for fold, (x_high, x_low) in zip(folds, x_tables):
        stacked = jnp.concatenate([fold[:, :HALF], fold[:, HALF:]], axis=0) * (1.0 / 512.0)
        high, low = halves(stacked)
        out = dot(x_high[...], high) + dot(x_high[...], low) + dot(x_low[...], high)
        parts.append(out.reshape(DEV, 8, HALF))
    return jnp.concatenate(parts, axis=1).astype(BF16)


def forward_kernel(
    counts, charges, splines, cells, y_high, y_low, even_high, even_low, odd_high, odd_low, out,
    left_ref, right_ref, row_ref, col_ref, total_ref,
):
    prepare(counts, charges, splines, cells, left_ref, right_ref, row_ref, col_ref)

    def plane_body(plane, carry):
        density_of(plane, left_ref, right_ref, row_ref, col_ref, total_ref)
        spectrum = plane_spectrum(
            total_ref[...], y_high, y_low, ((even_high, even_low), (odd_high, odd_low))
        )
        out[:, plane, 0] = spectrum[:, :, :128]
        out[:, plane, 1] = spectrum[:, :, 128:]
        return carry

    lax.fori_loop(0, SLAB, plane_body, 0)


def mix_kernel(green, shuffle, arrived, out, x_ref):
    first = lax.broadcasted_iota(jnp.int32, (NZ, 128), 1) == 0

    def turn(g, carry):
        at = pl.ds(g * 16, 16)
        block = jnp.concatenate(
            [arrived[at, 0].reshape(256, 128), arrived[at, 1].reshape(256, 128)], axis=1
        )
        x_ref[:, pl.ds(pl.multiple_of(g * 16, 16), 16), :] = (
            dot(shuffle[...], block).astype(BF16).reshape(16, 16, 256)
        )
        return carry

    lax.fori_loop(0, NZ // 16, turn, 0)

    def one_wave(parity, r):
        base = parity * 8 + r
        rows = [base, base + 2, base + 4, base + 6]
        pr, pi, mr, mi = (x_ref[row] for row in rows)
        p0 = [pr[:, :128].astype(F32), pi[:, :128].astype(F32)]
        m0 = [mr[:, :128].astype(F32), mi[:, :128].astype(F32)]
        m1 = [mr[:, 128:].astype(F32), mi[:, 128:].astype(F32)]
        zero = [(p0[0] + m0[0]) * 0.5, (p0[1] + m0[1]) * 0.5]
        last = [(p0[1] - m0[1]) * 0.5, (m0[0] - p0[0]) * 0.5]
        pick = lambda a, b: jnp.concatenate(
            [jnp.where(first, x, y) for x, y in zip(a, b)], axis=1
        ).astype(BF16)
        block0 = pick(zero, p0)
        block1 = jnp.concatenate([pr[:, 128:], pi[:, 128:]], axis=1)
        block2 = pick(last, m1)
        block3 = pick(m1, m0)
        u = 2 * r + parity
        y0, y1, y2, y3 = (
            dot(green[u, b], block) for b, block in enumerate((block0, block1, block2, block3))
        )
        re = lambda a: a[:, :128]
        im = lambda a: a[:, 128:]
        ar = jnp.where(first, (re(y0) - im(y2)) * 0.5, re(y0))
        ai = jnp.where(first, (im(y0) + re(y2)) * 0.5, im(y0))
        br = jnp.where(first, (re(y0) + im(y2)) * 0.5, re(y3))
        bi = jnp.where(first, (im(y0) - re(y2)) * 0.5, im(y3))
        cr = jnp.where(first, re(y3), re(y2))
        ci = jnp.where(first, im(y3), im(y2))
        x_ref[rows[0]] = jnp.concatenate([ar, re(y1)], axis=1).astype(BF16)
        x_ref[rows[1]] = jnp.concatenate([ai, im(y1)], axis=1).astype(BF16)
        x_ref[rows[2]] = jnp.concatenate([br, cr], axis=1).astype(BF16)
        x_ref[rows[3]] = jnp.concatenate([bi, ci], axis=1).astype(BF16)

    def wave_body(i, carry):
        one_wave(i // 2, i % 2)
        return carry

    lax.fori_loop(0, 4, wave_body, 0)

    def turn_back(g, carry):
        block = x_ref[:, pl.ds(pl.multiple_of(g * 16, 16), 16), :].reshape(256, 256)
        tiles = dot(shuffle[...], block).astype(BF16).reshape(16, 16, 256)
        at = pl.ds(g * 16, 16)
        out[at, 0] = tiles[:, :, :128]
        out[at, 1] = tiles[:, :, 128:]
        return carry

    lax.fori_loop(0, NZ // 16, turn_back, 0)


def inverse_kernel(arrived, y_high, even_high, odd_high, unzip, out, even_ref, odd_ref):
    even_t = even_high[...].T
    odd_t = odd_high[...].T

    def plane_body(plane, carry):
        def part(g, inner):
            at = pl.ds(g * 16, 16)
            block = jnp.concatenate(
                [arrived[at, plane, h].reshape(256, 128) for h in range(2)], axis=1
            )
            rows = dot(unzip[...], block).astype(BF16)
            to = pl.ds(pl.multiple_of(g * 128, 128), 128)
            even_ref[to, :] = rows[:128]
            odd_ref[to, :] = rows[128:]
            return inner

        lax.fori_loop(0, DEV // 16, part, 0)
        even = dot(even_t, even_ref[...])
        odd = dot(odd_t, odd_ref[...])
        lower, upper = even + odd, even - odd
        middle = jnp.concatenate(
            [
                jnp.concatenate([lower[:HALF], lower[HALF:]], axis=1),
                jnp.concatenate([upper[:HALF], upper[HALF:]], axis=1),
            ],
            axis=0,
        ).astype(BF16)
        out[plane] = dot_nt(middle, y_high[...]) * (1.0 / 512.0)
        return carry

    lax.fori_loop(0, SLAB, plane_body, 0)


def make_unzip():
    q, d, k = np.meshgrid(np.arange(2), np.arange(16), np.arange(8), indexing="ij")
    unzip = np.zeros((256, 256), np.float32)
    unzip[(q * 128 + d * 8 + k).reshape(-1), (d * 16 + q * 8 + k).reshape(-1)] = 1.0
    return unzip.astype(BF16)


VMEM = pl.BlockSpec(memory_space=pltpu.VMEM)
PARAMS = pltpu.CompilerParams(vmem_limit_bytes=60 * 2**20)


def shards(charges, cells, splines, counts, green):
    tables = make_tables()
    shuffle = make_shuffle()
    spectrum = pl.pallas_call(
        forward_kernel,
        out_shape=jax.ShapeDtypeStruct((DEV, SLAB, 2, 16, 128), BF16),
        in_specs=[pl.BlockSpec(memory_space=pltpu.SMEM)] + [VMEM] * 9,
        out_specs=VMEM,
        scratch_shapes=[
            pltpu.VMEM((SPREAD, SLOTS), F32),
            pltpu.VMEM((SPREAD, SLOTS), F32),
            pltpu.VMEM((SPREAD, SLOTS), jnp.int32),
            pltpu.VMEM((SPREAD, SLOTS), jnp.int32),
            pltpu.VMEM((NX, NY), F32),
        ],
        compiler_params=PARAMS,
        name="forward",
    )(counts, charges.reshape(1, SLOTS), splines, cells, *tables)
    arrived = lax.all_to_all(spectrum, ("zg", "xy"), split_axis=0, concat_axis=0, tiled=True)
    mixed = pl.pallas_call(
        mix_kernel,
        out_shape=jax.ShapeDtypeStruct((NZ, 2, 16, 128), BF16),
        in_specs=[VMEM] * 3,
        out_specs=VMEM,
        scratch_shapes=[pltpu.VMEM((16, NZ, 256), BF16)],
        compiler_params=PARAMS,
        name="mix",
    )(green, shuffle, arrived.reshape(NZ, 2, 16, 128))
    returned = lax.all_to_all(
        mixed.reshape(DEV, SLAB, 2, 16, 128), ("zg", "xy"), split_axis=0, concat_axis=0, tiled=True
    )
    return pl.pallas_call(
        inverse_kernel,
        out_shape=jax.ShapeDtypeStruct((SLAB, NX, NY), F32),
        in_specs=[VMEM] * 5,
        out_specs=VMEM,
        scratch_shapes=[pltpu.VMEM((DEV * 8, HALF), BF16), pltpu.VMEM((DEV * 8, HALF), BF16)],
        compiler_params=PARAMS,
        name="inverse",
    )(returned, tables[0], tables[2], tables[4], make_unzip())


def solution(mesh):
    in_specs = (
        P(("zg", "xy")),
        P(None, ("zg", "xy")),
        P(None, ("zg", "xy")),
        P(("zg", "xy")),
        P(("zg", "xy"), None, None, None),
    )
    out_specs = P(("zg", "xy"), None, None)
    return jax.shard_map(shards, mesh=mesh, in_specs=in_specs, out_specs=out_specs, check_vma=False)
```

```python
import functools
import math

import numpy as np
import jax
import jax.numpy as jnp
from jax import lax
from jax.experimental import pallas as pl
from jax.experimental.pallas import tpu as pltpu
from jax.sharding import PartitionSpec as P

NX = 512
NY = 512
NZ = 384
HALF = 256
DEV = 128
SLAB = 3
SLOTS = 2048
SPREAD = 8
CHUNK = 256
CANDIDATES = 32
STEP = 37
F32 = jnp.float32
BF16 = jnp.bfloat16


def split_table(table):
    high = table.astype(np.float32).astype(BF16)
    low = (table - high.astype(np.float64)).astype(np.float32).astype(BF16)
    return high, low


def make_tables():
    y = np.arange(NY)[:, None]
    v = np.arange(HALF)[None, :]
    angle = 2.0 * math.pi * (y * v % NY) / NY
    along_p = np.cos(angle)
    along_q = -np.sin(angle)
    along_q[:, 0] = 1.0 - 2.0 * (np.arange(NY) % 2)
    y_high, y_low = split_table(np.concatenate([along_p, along_q], axis=1))
    x = np.arange(HALF)[None, None, :]
    result = [y_high, y_low]
    for parity in range(2):
        u = (4 * np.arange(DEV)[:, None] + 2 * np.arange(2)[None, :] + parity)[:, :, None]
        angle = 2.0 * math.pi * (u * x % NX) / NX
        c, s = np.cos(angle), np.sin(angle)
        rows = [
            np.concatenate([c, s], axis=2),
            np.concatenate([-s, c], axis=2),
            np.concatenate([c, -s], axis=2),
            np.concatenate([-s, -c], axis=2),
        ]
        table = np.stack(rows, axis=1).reshape(DEV * 8, NX)
        result += split_table(table)
    return result


def make_shuffle():
    k, w = np.meshgrid(np.arange(16), np.arange(16), indexing="ij")
    shuffle = np.zeros((256, 256), np.float32)
    shuffle[(k * 16 + w).reshape(-1), (w * 16 + k).reshape(-1)] = 1.0
    return shuffle.astype(BF16)


def dot(a, b):
    return jnp.dot(a, b, preferred_element_type=F32)


def dot_nt(a, b):
    return lax.dot_general(a, b, (((1,), (1,)), ((), ())), preferred_element_type=F32)


def dot_tn(a, b):
    return lax.dot_general(a, b, (((0,), (0,)), ((), ())), preferred_element_type=F32)


def halves(value):
    high = value.astype(BF16)
    return high, (value - high.astype(F32)).astype(BF16)


def factor(value):
    best_left = jnp.ones_like(value)
    best_right = value.astype(BF16).astype(F32)
    best_error = jnp.abs(best_right - value)
    for j in range(1, CANDIDATES):
        left = 1.0 + j * (128 // CANDIDATES) / 128.0
        right = (value * (1.0 / left)).astype(BF16).astype(F32)
        error = jnp.abs(right * left - value)
        better = error < best_error
        best_error = jnp.where(better, error, best_error)
        best_right = jnp.where(better, right, best_right)
        best_left = jnp.where(better, left, best_left)
    return best_left, best_right


def prepare(counts, charges, splines, cells, left_ref, right_ref, row_ref, col_ref):
    slot = lax.broadcasted_iota(jnp.int32, (1, SLOTS), 1)
    live = jnp.where(slot < counts[0], charges[...], 0.0)
    left, right = factor(splines[...] * live)
    left_ref[...] = left
    right_ref[...] = right
    row_ref[...] = lax.shift_right_logical(cells[...], 9)
    col_ref[...] = lax.bitwise_and(cells[...], NY - 1)


def density_of(plane, left_ref, right_ref, row_ref, col_ref, total_ref):
    total_ref[...] = jnp.zeros_like(total_ref)
    index = lax.broadcasted_iota(jnp.int32, (NX, CHUNK), 0)
    index_row = index + plane * NX

    def body(c, carry):
        at = pl.ds(pl.multiple_of(c * CHUNK, CHUNK), CHUNK)
        a, b = [], []
        for k in range(SPREAD):
            a.append(jnp.where(row_ref[k : k + 1, at] == index_row, left_ref[k : k + 1, at], 0.0).astype(BF16))
            b.append(jnp.where(col_ref[k : k + 1, at] == index, right_ref[k : k + 1, at], 0.0).astype(BF16))
        total_ref[...] += dot_nt(jnp.concatenate(a, axis=1), jnp.concatenate(b, axis=1))
        return carry

    lax.fori_loop(0, SLOTS // CHUNK, body, 0)


def plane_spectrum(density, y_high, y_low, x_tables):
    high, low = halves(density)
    along = dot(high, y_high[...]) + dot(high, y_low[...]) + dot(low, y_high[...])
    folds = (along[:HALF] + along[HALF:], along[:HALF] - along[HALF:])
    parts = []
    for fold, (x_high, x_low) in zip(folds, x_tables):
        stacked = jnp.concatenate([fold[:, :HALF], fold[:, HALF:]], axis=0) * (1.0 / 512.0)
        high, low = halves(stacked)
        out = dot(x_high[...], high) + dot(x_high[...], low) + dot(x_low[...], high)
        parts.append(out.reshape(DEV, 8, HALF))
    return jnp.concatenate(parts, axis=1).astype(BF16)


def make_unzip():
    q, d, k = np.meshgrid(np.arange(2), np.arange(16), np.arange(8), indexing="ij")
    unzip = np.zeros((256, 256), np.float32)
    unzip[(q * 128 + d * 8 + k).reshape(-1), (d * 16 + q * 8 + k).reshape(-1)] = 1.0
    return unzip.astype(BF16)


def peer_of(me, i):
    return lax.rem(me + STEP * i, DEV)


def place(device):
    return (device // 64, lax.rem(device, 64))


def fused_kernel(
    counts, charges, splines, cells, shuffle, unzip, *rest,
):
    sources, middle = rest[:7], rest[7]
    left_ref, right_ref, row_ref, col_ref, total_ref = rest[8:13]
    held, (green,) = rest[13:19], rest[19:20]
    send1, arrive1, x_ref, send2, arrive2, even_ref, odd_ref, even_t, odd_t = rest[20:29]
    load_sem, send_sem, arrive1_sem, arrive2_sem = rest[29:33]
    y_high, y_low, even_high, even_low, odd_high, odd_low = held
    me = lax.axis_index("zg") * 64 + lax.axis_index("xy")

    barrier = pltpu.get_barrier_semaphore()

    def greet(i, carry):
        pl.semaphore_signal(
            barrier, inc=1, device_id=place(peer_of(me, i)), device_id_type=pl.DeviceIdType.MESH
        )
        return carry

    lax.fori_loop(1, DEV, greet, 0)
    loads = [
        pltpu.make_async_copy(source, target, load_sem.at[i])
        for i, (source, target) in enumerate(zip(sources, (*held, green)))
    ]
    for load in loads:
        load.start()
    prepare(counts, charges, splines, cells, left_ref, right_ref, row_ref, col_ref)

    def plane_body(plane, carry):
        density_of(plane, left_ref, right_ref, row_ref, col_ref, total_ref)

        @pl.when(plane == 0)
        def _():
            for load in loads[:6]:
                load.wait()
            pl.semaphore_wait(barrier, DEV - 1)

        spectrum = plane_spectrum(
            total_ref[...], y_high, y_low, ((even_high, even_low), (odd_high, odd_low))
        )
        send1[plane, :, 0] = spectrum[:, :, :128]
        send1[plane, :, 1] = spectrum[:, :, 128:]

        def send(i, inner):
            peer = peer_of(me, i)
            pltpu.make_async_remote_copy(
                src_ref=send1.at[plane, peer],
                dst_ref=arrive1.at[me, plane],
                send_sem=send_sem.at[0],
                recv_sem=arrive1_sem,
                device_id=place(peer),
                device_id_type=pl.DeviceIdType.MESH,
            ).start()
            return inner

        lax.fori_loop(1, DEV, send, 0)
        arrive1[me, plane] = send1[plane, me]
        return carry

    lax.fori_loop(0, SLAB, plane_body, 0)
    even_t[...] = even_high[...].T
    odd_t[...] = odd_high[...].T
    loads[6].wait()
    most = arrive1.at[pl.ds(0, DEV - 1)]
    pltpu.make_async_copy(most, most, arrive1_sem).wait()

    mix(green, shuffle, arrive1, send2, x_ref)

    for plane in range(SLAB):

        def send(i, inner):
            peer = peer_of(me, i)
            pltpu.make_async_remote_copy(
                src_ref=send2.at[peer, plane],
                dst_ref=arrive2.at[plane, me],
                send_sem=send_sem.at[1],
                recv_sem=arrive2_sem.at[plane],
                device_id=place(peer),
                device_id_type=pl.DeviceIdType.MESH,
            ).start()
            return inner

        lax.fori_loop(1, DEV, send, 0)
        arrive2[plane, me] = send2[me, plane]

    for plane in range(SLAB):
        most = arrive2.at[plane, pl.ds(0, DEV - 1)]
        pltpu.make_async_copy(most, most, arrive2_sem.at[plane]).wait()
        middle[plane] = back_along_x(arrive2, plane, unzip, even_t, odd_t, even_ref, odd_ref)

    most = arrive1.at[pl.ds(0, DEV - 1)]
    for i in range(2):
        pltpu.make_async_copy(most, most, send_sem.at[i]).wait()


def mix(green, shuffle, arrived, out, x_ref):
    first = lax.broadcasted_iota(jnp.int32, (NZ, 128), 1) == 0

    def turn(g, carry):
        at = pl.ds(g * 16, 16)
        for j in range(3):
            block = jnp.concatenate(
                [
                    arrived[at, :, h].reshape(48, 16, 128)[16 * j : 16 * j + 16].reshape(256, 128)
                    for h in range(2)
                ],
                axis=1,
            )
            x_ref[:, pl.ds(pl.multiple_of(g * 48 + j * 16, 16), 16), :] = (
                dot(shuffle[...], block).astype(BF16).reshape(16, 16, 256)
            )
        return carry

    lax.fori_loop(0, DEV // 16, turn, 0)

    def one_wave(parity, r):
        base = parity * 8 + r
        rows = [base, base + 2, base + 4, base + 6]
        pr, pi, mr, mi = (x_ref[row] for row in rows)
        p0 = [pr[:, :128].astype(F32), pi[:, :128].astype(F32)]
        m0 = [mr[:, :128].astype(F32), mi[:, :128].astype(F32)]
        m1 = [mr[:, 128:].astype(F32), mi[:, 128:].astype(F32)]
        zero = [(p0[0] + m0[0]) * 0.5, (p0[1] + m0[1]) * 0.5]
        last = [(p0[1] - m0[1]) * 0.5, (m0[0] - p0[0]) * 0.5]
        pick = lambda a, b: jnp.concatenate(
            [jnp.where(first, x, y) for x, y in zip(a, b)], axis=1
        ).astype(BF16)
        block0 = pick(zero, p0)
        block1 = jnp.concatenate([pr[:, 128:], pi[:, 128:]], axis=1)
        block2 = pick(last, m1)
        block3 = pick(m1, m0)
        u = 2 * r + parity
        y0, y1, y2, y3 = (
            dot(green[u, b], block) for b, block in enumerate((block0, block1, block2, block3))
        )
        re = lambda a: a[:, :128]
        im = lambda a: a[:, 128:]
        ar = jnp.where(first, (re(y0) - im(y2)) * 0.5, re(y0))
        ai = jnp.where(first, (im(y0) + re(y2)) * 0.5, im(y0))
        br = jnp.where(first, (re(y0) + im(y2)) * 0.5, re(y3))
        bi = jnp.where(first, (im(y0) - re(y2)) * 0.5, im(y3))
        cr = jnp.where(first, re(y3), re(y2))
        ci = jnp.where(first, im(y3), im(y2))
        x_ref[rows[0]] = jnp.concatenate([ar, re(y1)], axis=1).astype(BF16)
        x_ref[rows[1]] = jnp.concatenate([ai, im(y1)], axis=1).astype(BF16)
        x_ref[rows[2]] = jnp.concatenate([br, cr], axis=1).astype(BF16)
        x_ref[rows[3]] = jnp.concatenate([bi, ci], axis=1).astype(BF16)

    def wave_body(i, carry):
        one_wave(i // 2, i % 2)
        return carry

    lax.fori_loop(0, 4, wave_body, 0)

    def turn_back(g, carry):
        tiles = []
        for j in range(3):
            block = x_ref[:, pl.ds(pl.multiple_of(g * 48 + j * 16, 16), 16), :].reshape(256, 256)
            tiles.append(dot(shuffle[...], block).astype(BF16).reshape(16, 16, 256))
        tiles = jnp.concatenate(tiles, axis=0).reshape(16, SLAB, 16, 256)
        at = pl.ds(g * 16, 16)
        out[at, :, 0] = tiles[..., :128]
        out[at, :, 1] = tiles[..., 128:]
        return carry

    lax.fori_loop(0, DEV // 16, turn_back, 0)


def back_along_x(arrived, plane, unzip, even_t, odd_t, even_ref, odd_ref):
    def part(g, inner):
        for j in range(2):
            at = pl.ds(g * 32 + j * 16, 16)
            block = jnp.concatenate(
                [arrived[plane, at, h].reshape(256, 128) for h in range(2)], axis=1
            )
            rows = dot(unzip[...], block).astype(BF16)
            to = pl.ds(pl.multiple_of(g * 256 + j * 128, 128), 128)
            even_ref[to, :] = rows[:128]
            odd_ref[to, :] = rows[128:]
        return inner

    lax.fori_loop(0, DEV // 32, part, 0)
    even = dot(even_t[...], even_ref[...])
    odd = dot(odd_t[...], odd_ref[...])
    lower, upper = even + odd, even - odd
    return jnp.concatenate(
        [
            jnp.concatenate([lower[:HALF], lower[HALF:]], axis=1),
            jnp.concatenate([upper[:HALF], upper[HALF:]], axis=1),
        ],
        axis=0,
    ).astype(BF16)


def back_along_y(middle, y_high, out):
    out[0] = dot_nt(middle[0], y_high[...]) * (1.0 / 512.0)


VMEM = pl.BlockSpec(memory_space=pltpu.VMEM)
ANY = pl.BlockSpec(memory_space=pl.ANY)


def shards(charges, cells, splines, counts, green):
    tables = make_tables()
    middle = pl.pallas_call(
        fused_kernel,
        out_shape=jax.ShapeDtypeStruct((SLAB, NX, NY), BF16),
        in_specs=[pl.BlockSpec(memory_space=pltpu.SMEM)] + [VMEM] * 5 + [ANY] * 7,
        out_specs=VMEM,
        scratch_shapes=[
            pltpu.VMEM((SPREAD, SLOTS), F32),
            pltpu.VMEM((SPREAD, SLOTS), F32),
            pltpu.VMEM((SPREAD, SLOTS), jnp.int32),
            pltpu.VMEM((SPREAD, SLOTS), jnp.int32),
            pltpu.VMEM((NX, NY), F32),
            *[pltpu.VMEM(table.shape, BF16) for table in tables],
            pltpu.VMEM(green.shape, BF16),
            pltpu.VMEM((SLAB, DEV, 2, 16, 128), BF16),
            pltpu.VMEM((DEV, SLAB, 2, 16, 128), BF16),
            pltpu.VMEM((16, NZ, 256), BF16),
            pltpu.VMEM((DEV, SLAB, 2, 16, 128), BF16),
            pltpu.VMEM((SLAB, DEV, 2, 16, 128), BF16),
            pltpu.VMEM((DEV * 8, HALF), BF16),
            pltpu.VMEM((DEV * 8, HALF), BF16),
            pltpu.VMEM((NX, DEV * 8), BF16),
            pltpu.VMEM((NX, DEV * 8), BF16),
            pltpu.SemaphoreType.DMA((7,)),
            pltpu.SemaphoreType.DMA((2,)),
            pltpu.SemaphoreType.DMA,
            pltpu.SemaphoreType.DMA((SLAB,)),
        ],
        compiler_params=pltpu.CompilerParams(
            collective_id=0, has_side_effects=True, vmem_limit_bytes=60 * 2**20
        ),
        name="fused",
    )(counts, charges.reshape(1, SLOTS), splines, cells, make_shuffle(), make_unzip(), *tables, green)
    return pl.pallas_call(
        back_along_y,
        grid=(SLAB,),
        out_shape=jax.ShapeDtypeStruct((SLAB, NX, NY), F32),
        in_specs=[
            pl.BlockSpec((1, NX, NY), lambda i: (i, 0, 0)),
            pl.BlockSpec((NY, NY), lambda i: (0, 0)),
        ],
        out_specs=pl.BlockSpec((1, NX, NY), lambda i: (i, 0, 0)),
        name="back_along_y",
    )(middle, tables[0])


def solution(mesh):
    in_specs = (
        P(("zg", "xy")),
        P(None, ("zg", "xy")),
        P(None, ("zg", "xy")),
        P(("zg", "xy")),
        P(("zg", "xy"), None, None, None),
    )
    out_specs = P(("zg", "xy"), None, None)
    return jax.shard_map(shards, mesh=mesh, in_specs=in_specs, out_specs=out_specs, check_vma=False)
```

```python
import functools
import math

import numpy as np
import jax
import jax.numpy as jnp
from jax import lax
from jax.experimental import pallas as pl
from jax.experimental.pallas import tpu as pltpu
from jax.sharding import PartitionSpec as P

NX = 512
NY = 512
NZ = 384
HALF = 256
DEV = 128
SLAB = 3
SLOTS = 2048
SPREAD = 8
CHUNK = 1024
CANDIDATES = 32
STEP = 37
GROUP = 9
F32 = jnp.float32
BF16 = jnp.bfloat16


def split_table(table):
    high = table.astype(np.float32).astype(BF16)
    low = (table - high.astype(np.float64)).astype(np.float32).astype(BF16)
    return high, low


def make_tables():
    y = np.arange(NY)[:, None]
    v = np.arange(HALF)[None, :]
    angle = 2.0 * math.pi * (y * v % NY) / NY
    along_p = np.cos(angle)
    along_q = -np.sin(angle)
    along_q[:, 0] = 1.0 - 2.0 * (np.arange(NY) % 2)
    y_high, y_low = split_table(np.concatenate([along_p, along_q], axis=1))
    x = np.arange(HALF)[None, None, :]
    result = [y_high, y_low]
    for parity in range(2):
        u = (4 * np.arange(DEV)[:, None] + 2 * np.arange(2)[None, :] + parity)[:, :, None]
        angle = 2.0 * math.pi * (u * x % NX) / NX
        c, s = np.cos(angle), np.sin(angle)
        rows = [
            np.concatenate([c, s], axis=2),
            np.concatenate([-s, c], axis=2),
            np.concatenate([c, -s], axis=2),
            np.concatenate([-s, -c], axis=2),
        ]
        table = np.stack(rows, axis=1).reshape(DEV * 8, NX)
        result += split_table(table)
    return result


def make_shuffle():
    k, w = np.meshgrid(np.arange(16), np.arange(16), indexing="ij")
    shuffle = np.zeros((256, 256), np.float32)
    shuffle[(k * 16 + w).reshape(-1), (w * 16 + k).reshape(-1)] = 1.0
    return shuffle.astype(BF16)


def dot(a, b):
    return jnp.dot(a, b, preferred_element_type=F32)


def dot_nt(a, b):
    return lax.dot_general(a, b, (((1,), (1,)), ((), ())), preferred_element_type=F32)


def dot_tn(a, b):
    return lax.dot_general(a, b, (((0,), (0,)), ((), ())), preferred_element_type=F32)


def halves(value):
    high = value.astype(BF16)
    return high, (value - high.astype(F32)).astype(BF16)


def factor(value):
    best_left = jnp.ones_like(value)
    best_right = value.astype(BF16).astype(F32)
    best_error = jnp.abs(best_right - value)
    for j in range(1, CANDIDATES):
        left = 1.0 + j * (128 // CANDIDATES) / 128.0
        right = (value * (1.0 / left)).astype(BF16).astype(F32)
        error = jnp.abs(right * left - value)
        better = error < best_error
        best_error = jnp.where(better, error, best_error)
        best_right = jnp.where(better, right, best_right)
        best_left = jnp.where(better, left, best_left)
    return best_left, best_right


def prepare(counts, charges, splines, cells, left_ref, right_ref, row_ref, col_ref):
    slot = lax.broadcasted_iota(jnp.int32, (1, SLOTS), 1)
    live = jnp.where(slot < counts[0], charges[...], 0.0)
    left, right = factor(splines[...] * live)
    left_ref[...] = left
    right_ref[...] = right
    row_ref[...] = lax.shift_right_logical(cells[...], 9)
    col_ref[...] = lax.bitwise_and(cells[...], NY - 1)


def density_of(plane, left_ref, right_ref, row_ref, col_ref, total_ref):
    total_ref[...] = jnp.zeros_like(total_ref)
    index = lax.broadcasted_iota(jnp.int32, (NX, CHUNK), 0)
    index_row = index + plane * NX

    def body(c, carry):
        at = pl.ds(pl.multiple_of(c * CHUNK, CHUNK), CHUNK)
        a, b = [], []
        for k in range(SPREAD):
            a.append(jnp.where(row_ref[k : k + 1, at] == index_row, left_ref[k : k + 1, at], 0.0).astype(BF16))
            b.append(jnp.where(col_ref[k : k + 1, at] == index, right_ref[k : k + 1, at], 0.0).astype(BF16))
        total_ref[...] += dot_nt(jnp.concatenate(a, axis=1), jnp.concatenate(b, axis=1))
        return carry

    lax.fori_loop(0, SLOTS // CHUNK, body, 0)


def plane_spectrum(density, y_high, y_low, x_tables):
    high, low = halves(density)
    along = dot(high, y_high[...]) + dot(high, y_low[...]) + dot(low, y_high[...])
    folds = (along[:HALF] + along[HALF:], along[:HALF] - along[HALF:])
    parts = []
    for fold, (x_high, x_low) in zip(folds, x_tables):
        stacked = jnp.concatenate([fold[:, :HALF], fold[:, HALF:]], axis=0) * (1.0 / 512.0)
        high, low = halves(stacked)
        out = dot(x_high[...], high) + dot(x_high[...], low) + dot(x_low[...], high)
        parts.append(out.reshape(DEV, 8, HALF))
    return jnp.concatenate(parts, axis=1).astype(BF16)


def make_unzip():
    q, d, k = np.meshgrid(np.arange(2), np.arange(16), np.arange(8), indexing="ij")
    unzip = np.zeros((256, 256), np.float32)
    unzip[(q * 128 + d * 8 + k).reshape(-1), (d * 16 + q * 8 + k).reshape(-1)] = 1.0
    return unzip.astype(BF16)


def peer_of(me, i):
    return lax.rem(me + STEP * i, DEV)


def each_peer(me, action):
    def several(j, carry):
        for k in range(GROUP):
            action(peer_of(me, 1 + GROUP * j + k))
        return carry

    lax.fori_loop(0, (DEV - 2) // GROUP, several, 0)
    action(peer_of(me, DEV - 1))


def place(device):
    return (device // 64, lax.rem(device, 64))


def fused_kernel(
    counts, charges, splines, cells, shuffle, unzip, *rest,
):
    sources, middle = rest[:7], rest[7]
    left_ref, right_ref, row_ref, col_ref, total_ref = rest[8:13]
    held, (green,) = rest[13:19], rest[19:20]
    send1, arrive1, x_ref, send2, arrive2, even_ref, odd_ref, even_t, odd_t = rest[20:29]
    load_sem, send_sem, arrive1_sem, arrive2_sem = rest[29:33]
    y_high, y_low, even_high, even_low, odd_high, odd_low = held
    me = lax.axis_index("zg") * 64 + lax.axis_index("xy")

    barrier = pltpu.get_barrier_semaphore()

    def greet(peer):
        pl.semaphore_signal(
            barrier, inc=1, device_id=place(peer), device_id_type=pl.DeviceIdType.MESH
        )

    loads = [
        pltpu.make_async_copy(source, target, load_sem.at[i])
        for i, (source, target) in enumerate(zip(sources, (*held, green)))
    ]
    for load in loads:
        load.start()
    each_peer(me, greet)
    prepare(counts, charges, splines, cells, left_ref, right_ref, row_ref, col_ref)

    def plane_body(plane, carry):
        density_of(plane, left_ref, right_ref, row_ref, col_ref, total_ref)

        @pl.when(plane == 0)
        def _():
            for load in loads[:6]:
                load.wait()
            pl.semaphore_wait(barrier, DEV - 1)

        spectrum = plane_spectrum(
            total_ref[...], y_high, y_low, ((even_high, even_low), (odd_high, odd_low))
        )
        send1[plane, :, 0] = spectrum[:, :, :128]
        send1[plane, :, 1] = spectrum[:, :, 128:]

        def send(peer):
            pltpu.make_async_remote_copy(
                src_ref=send1.at[plane, peer],
                dst_ref=arrive1.at[me, plane],
                send_sem=send_sem.at[0],
                recv_sem=arrive1_sem,
                device_id=place(peer),
                device_id_type=pl.DeviceIdType.MESH,
            ).start()

        each_peer(me, send)
        arrive1[me, plane] = send1[plane, me]
        return carry

    lax.fori_loop(0, SLAB, plane_body, 0)
    even_t[...] = even_high[...].T
    odd_t[...] = odd_high[...].T
    loads[6].wait()
    most = arrive1.at[pl.ds(0, DEV - 1)]
    pltpu.make_async_copy(most, most, arrive1_sem).wait()

    mix(green, shuffle, arrive1, send2, x_ref)

    for plane in range(SLAB):

        def send(peer):
            pltpu.make_async_remote_copy(
                src_ref=send2.at[peer, plane],
                dst_ref=arrive2.at[plane, me],
                send_sem=send_sem.at[1],
                recv_sem=arrive2_sem.at[plane],
                device_id=place(peer),
                device_id_type=pl.DeviceIdType.MESH,
            ).start()

        each_peer(me, send)
        arrive2[plane, me] = send2[me, plane]

    for plane in range(SLAB):
        most = arrive2.at[plane, pl.ds(0, DEV - 1)]
        pltpu.make_async_copy(most, most, arrive2_sem.at[plane]).wait()
        middle[plane] = back_along_x(arrive2, plane, unzip, even_t, odd_t, even_ref, odd_ref)

    most = arrive1.at[pl.ds(0, DEV - 1)]
    for i in range(2):
        pltpu.make_async_copy(most, most, send_sem.at[i]).wait()


def mix(green, shuffle, arrived, out, x_ref):
    first = lax.broadcasted_iota(jnp.int32, (NZ, 128), 1) == 0

    def turn(g, carry):
        at = pl.ds(g * 16, 16)
        for j in range(3):
            block = jnp.concatenate(
                [
                    arrived[at, :, h].reshape(48, 16, 128)[16 * j : 16 * j + 16].reshape(256, 128)
                    for h in range(2)
                ],
                axis=1,
            )
            x_ref[:, pl.ds(pl.multiple_of(g * 48 + j * 16, 16), 16), :] = (
                dot(shuffle[...], block).astype(BF16).reshape(16, 16, 256)
            )
        return carry

    lax.fori_loop(0, DEV // 16, turn, 0, unroll=8)

    def one_wave(parity, r):
        base = parity * 8 + r
        rows = [base, base + 2, base + 4, base + 6]
        pr, pi, mr, mi = (x_ref[row] for row in rows)
        p0 = [pr[:, :128].astype(F32), pi[:, :128].astype(F32)]
        m0 = [mr[:, :128].astype(F32), mi[:, :128].astype(F32)]
        m1 = [mr[:, 128:].astype(F32), mi[:, 128:].astype(F32)]
        zero = [(p0[0] + m0[0]) * 0.5, (p0[1] + m0[1]) * 0.5]
        last = [(p0[1] - m0[1]) * 0.5, (m0[0] - p0[0]) * 0.5]
        pick = lambda a, b: jnp.concatenate(
            [jnp.where(first, x, y) for x, y in zip(a, b)], axis=1
        ).astype(BF16)
        block0 = pick(zero, p0)
        block1 = jnp.concatenate([pr[:, 128:], pi[:, 128:]], axis=1)
        block2 = pick(last, m1)
        block3 = pick(m1, m0)
        u = 2 * r + parity
        y0, y1, y2, y3 = (
            dot(green[u, b], block) for b, block in enumerate((block0, block1, block2, block3))
        )
        re = lambda a: a[:, :128]
        im = lambda a: a[:, 128:]
        ar = jnp.where(first, (re(y0) - im(y2)) * 0.5, re(y0))
        ai = jnp.where(first, (im(y0) + re(y2)) * 0.5, im(y0))
        br = jnp.where(first, (re(y0) + im(y2)) * 0.5, re(y3))
        bi = jnp.where(first, (im(y0) - re(y2)) * 0.5, im(y3))
        cr = jnp.where(first, re(y3), re(y2))
        ci = jnp.where(first, im(y3), im(y2))
        x_ref[rows[0]] = jnp.concatenate([ar, re(y1)], axis=1).astype(BF16)
        x_ref[rows[1]] = jnp.concatenate([ai, im(y1)], axis=1).astype(BF16)
        x_ref[rows[2]] = jnp.concatenate([br, cr], axis=1).astype(BF16)
        x_ref[rows[3]] = jnp.concatenate([bi, ci], axis=1).astype(BF16)

    def wave_body(i, carry):
        one_wave(i // 2, i % 2)
        return carry

    lax.fori_loop(0, 4, wave_body, 0, unroll=4)

    def turn_back(g, carry):
        tiles = []
        for j in range(3):
            block = x_ref[:, pl.ds(pl.multiple_of(g * 48 + j * 16, 16), 16), :].reshape(256, 256)
            tiles.append(dot(shuffle[...], block).astype(BF16).reshape(16, 16, 256))
        tiles = jnp.concatenate(tiles, axis=0).reshape(16, SLAB, 16, 256)
        at = pl.ds(g * 16, 16)
        out[at, :, 0] = tiles[..., :128]
        out[at, :, 1] = tiles[..., 128:]
        return carry

    lax.fori_loop(0, DEV // 16, turn_back, 0, unroll=8)


def back_along_x(arrived, plane, unzip, even_t, odd_t, even_ref, odd_ref):
    def part(g, inner):
        for j in range(2):
            at = pl.ds(g * 32 + j * 16, 16)
            block = jnp.concatenate(
                [arrived[plane, at, h].reshape(256, 128) for h in range(2)], axis=1
            )
            rows = dot(unzip[...], block).astype(BF16)
            to = pl.ds(pl.multiple_of(g * 256 + j * 128, 128), 128)
            even_ref[to, :] = rows[:128]
            odd_ref[to, :] = rows[128:]
        return inner

    lax.fori_loop(0, DEV // 32, part, 0, unroll=4)
    even = dot(even_t[...], even_ref[...])
    odd = dot(odd_t[...], odd_ref[...])
    lower, upper = even + odd, even - odd
    return jnp.concatenate(
        [
            jnp.concatenate([lower[:HALF], lower[HALF:]], axis=1),
            jnp.concatenate([upper[:HALF], upper[HALF:]], axis=1),
        ],
        axis=0,
    ).astype(BF16)


def back_along_y(middle, y_high, out):
    out[0] = dot_nt(middle[0], y_high[...]) * (1.0 / 512.0)


VMEM = pl.BlockSpec(memory_space=pltpu.VMEM)
ANY = pl.BlockSpec(memory_space=pl.ANY)


def shards(charges, cells, splines, counts, green):
    tables = make_tables()
    middle = pl.pallas_call(
        fused_kernel,
        out_shape=jax.ShapeDtypeStruct((SLAB, NX, NY), BF16),
        in_specs=[pl.BlockSpec(memory_space=pltpu.SMEM)] + [VMEM] * 5 + [ANY] * 7,
        out_specs=VMEM,
        scratch_shapes=[
            pltpu.VMEM((SPREAD, SLOTS), F32),
            pltpu.VMEM((SPREAD, SLOTS), F32),
            pltpu.VMEM((SPREAD, SLOTS), jnp.int32),
            pltpu.VMEM((SPREAD, SLOTS), jnp.int32),
            pltpu.VMEM((NX, NY), F32),
            *[pltpu.VMEM(table.shape, BF16) for table in tables],
            pltpu.VMEM(green.shape, BF16),
            pltpu.VMEM((SLAB, DEV, 2, 16, 128), BF16),
            pltpu.VMEM((DEV, SLAB, 2, 16, 128), BF16),
            pltpu.VMEM((16, NZ, 256), BF16),
            pltpu.VMEM((DEV, SLAB, 2, 16, 128), BF16),
            pltpu.VMEM((SLAB, DEV, 2, 16, 128), BF16),
            pltpu.VMEM((DEV * 8, HALF), BF16),
            pltpu.VMEM((DEV * 8, HALF), BF16),
            pltpu.VMEM((NX, DEV * 8), BF16),
            pltpu.VMEM((NX, DEV * 8), BF16),
            pltpu.SemaphoreType.DMA((7,)),
            pltpu.SemaphoreType.DMA((2,)),
            pltpu.SemaphoreType.DMA,
            pltpu.SemaphoreType.DMA((SLAB,)),
        ],
        compiler_params=pltpu.CompilerParams(
            collective_id=0, has_side_effects=True, vmem_limit_bytes=60 * 2**20
        ),
        name="fused",
    )(counts, charges.reshape(1, SLOTS), splines, cells, make_shuffle(), make_unzip(), *tables, green)
    return pl.pallas_call(
        back_along_y,
        grid=(SLAB,),
        out_shape=jax.ShapeDtypeStruct((SLAB, NX, NY), F32),
        in_specs=[
            pl.BlockSpec((1, NX, NY), lambda i: (i, 0, 0)),
            pl.BlockSpec((NY, NY), lambda i: (0, 0)),
        ],
        out_specs=pl.BlockSpec((1, NX, NY), lambda i: (i, 0, 0)),
        name="back_along_y",
    )(middle, tables[0])


def solution(mesh):
    in_specs = (
        P(("zg", "xy")),
        P(None, ("zg", "xy")),
        P(None, ("zg", "xy")),
        P(("zg", "xy")),
        P(("zg", "xy"), None, None, None),
    )
    out_specs = P(("zg", "xy"), None, None)
    return jax.shard_map(shards, mesh=mesh, in_specs=in_specs, out_specs=out_specs, check_vma=False)
```

```python
import functools
import math

import numpy as np
import jax
import jax.numpy as jnp
from jax import lax
from jax.experimental import pallas as pl
from jax.experimental.pallas import tpu as pltpu
from jax.sharding import PartitionSpec as P

NX = 512
NY = 512
NZ = 384
HALF = 256
DEV = 128
SLAB = 3
SLOTS = 2048
SPREAD = 8
CHUNK = 1024
CANDIDATES = 32
STEP = 37
GROUP = 9
F32 = jnp.float32
BF16 = jnp.bfloat16


def split_table(table):
    high = table.astype(np.float32).astype(BF16)
    low = (table - high.astype(np.float64)).astype(np.float32).astype(BF16)
    return high, low


def make_tables():
    y = np.arange(NY)[:, None]
    v = np.arange(HALF)[None, :]
    angle = 2.0 * math.pi * (y * v % NY) / NY
    along_p = np.cos(angle)
    along_q = -np.sin(angle)
    along_q[:, 0] = 1.0 - 2.0 * (np.arange(NY) % 2)
    y_high, y_low = split_table(np.concatenate([along_p, along_q], axis=1))
    x = np.arange(HALF)[None, None, :]
    result = [y_high, y_low]
    for parity in range(2):
        u = (4 * np.arange(DEV)[:, None] + 2 * np.arange(2)[None, :] + parity)[:, :, None]
        angle = 2.0 * math.pi * (u * x % NX) / NX
        c, s = np.cos(angle), np.sin(angle)
        rows = [
            np.concatenate([c, s], axis=2),
            np.concatenate([-s, c], axis=2),
            np.concatenate([c, -s], axis=2),
            np.concatenate([-s, -c], axis=2),
        ]
        table = np.stack(rows, axis=1).reshape(DEV * 8, NX)
        result += split_table(table)
    return result


def make_shuffle():
    k, w = np.meshgrid(np.arange(16), np.arange(16), indexing="ij")
    shuffle = np.zeros((256, 256), np.float32)
    shuffle[(k * 16 + w).reshape(-1), (w * 16 + k).reshape(-1)] = 1.0
    return shuffle.astype(BF16)


def dot(a, b):
    return jnp.dot(a, b, preferred_element_type=F32)


def dot_nt(a, b):
    return lax.dot_general(a, b, (((1,), (1,)), ((), ())), preferred_element_type=F32)


def dot_tn(a, b):
    return lax.dot_general(a, b, (((0,), (0,)), ((), ())), preferred_element_type=F32)


def halves(value):
    high = value.astype(BF16)
    return high, (value - high.astype(F32)).astype(BF16)


def factor(value):
    best_left = jnp.ones_like(value)
    best_right = value.astype(BF16).astype(F32)
    best_error = jnp.abs(best_right - value)
    for j in range(1, CANDIDATES):
        left = 1.0 + j * (128 // CANDIDATES) / 128.0
        right = (value * (1.0 / left)).astype(BF16).astype(F32)
        error = jnp.abs(right * left - value)
        better = error < best_error
        best_error = jnp.where(better, error, best_error)
        best_right = jnp.where(better, right, best_right)
        best_left = jnp.where(better, left, best_left)
    return best_left, best_right


def prepare(counts, charges, splines, cells, left_ref, right_ref, row_ref, col_ref):
    slot = lax.broadcasted_iota(jnp.int32, (1, SLOTS), 1)
    live = jnp.where(slot < counts[0], charges[...], 0.0)
    left, right = factor(splines[...] * live)
    left_ref[...] = left
    right_ref[...] = right
    row_ref[...] = lax.shift_right_logical(cells[...], 9)
    col_ref[...] = lax.bitwise_and(cells[...], NY - 1)


def density_of(plane, left_ref, right_ref, row_ref, col_ref, total_ref):
    total_ref[...] = jnp.zeros_like(total_ref)
    index = lax.broadcasted_iota(jnp.int32, (NX, CHUNK), 0)
    index_row = index + plane * NX

    def body(c, carry):
        at = pl.ds(pl.multiple_of(c * CHUNK, CHUNK), CHUNK)
        a, b = [], []
        for k in range(SPREAD):
            a.append(jnp.where(row_ref[k : k + 1, at] == index_row, left_ref[k : k + 1, at], 0.0).astype(BF16))
            b.append(jnp.where(col_ref[k : k + 1, at] == index, right_ref[k : k + 1, at], 0.0).astype(BF16))
        total_ref[...] += dot_nt(jnp.concatenate(a, axis=1), jnp.concatenate(b, axis=1))
        return carry

    lax.fori_loop(0, SLOTS // CHUNK, body, 0)


def along_y(density, y_high, y_low):
    high, low = halves(density)
    along = dot(high, y_high[...]) + dot(high, y_low[...]) + dot(low, y_high[...])
    return along[:HALF] + along[HALF:], along[:HALF] - along[HALF:]


def along_x(fold, x_high, x_low):
    stacked = jnp.concatenate([fold[:, :HALF], fold[:, HALF:]], axis=0) * (1.0 / 512.0)
    high, low = halves(stacked)
    out = dot(x_high[...], high) + dot(x_high[...], low) + dot(x_low[...], high)
    out = out.reshape(DEV, 8, HALF)
    return jnp.concatenate([out[:, :, :128], out[:, :, 128:]], axis=1).astype(BF16)


def make_unzip():
    q, d, k = np.meshgrid(np.arange(2), np.arange(16), np.arange(8), indexing="ij")
    unzip = np.zeros((256, 256), np.float32)
    unzip[(q * 128 + d * 8 + k).reshape(-1), (d * 16 + q * 8 + k).reshape(-1)] = 1.0
    return unzip.astype(BF16)


def peer_of(me, i):
    return lax.rem(me + STEP * i, DEV)


def each_peer(me, action):
    def several(j, carry):
        for k in range(GROUP):
            action(peer_of(me, 1 + GROUP * j + k))
        return carry

    lax.fori_loop(0, (DEV - 2) // GROUP, several, 0)
    action(peer_of(me, DEV - 1))


def place(device):
    return (device // 64, lax.rem(device, 64))


def fused_kernel(counts, charges, splines, cells, *rest):
    sources, out = rest[:9], rest[9]
    lists, total_ref = rest[10:14], rest[14]
    held = rest[15:24]
    send1, arrive1, x_ref, send2, arrive2, turned, transposed, halfway, stage = rest[24:33]
    load_sem, send_sem, arrive1_sem, arrive2_sem, out_sem = rest[33:38]
    y_high, y_low, even_high, even_low, odd_high, odd_low, shuffle, unzip, green = held
    me = lax.axis_index("zg") * 64 + lax.axis_index("xy")
    barrier = pltpu.get_barrier_semaphore()

    loads = [
        pltpu.make_async_copy(source, target, load_sem.at[i])
        for i, (source, target) in enumerate(zip(sources, held))
    ]
    for load in loads:
        load.start()

    def greet(peer):
        pl.semaphore_signal(
            barrier, inc=1, device_id=place(peer), device_id_type=pl.DeviceIdType.MESH
        )

    each_peer(me, greet)
    prepare(counts, charges, splines, cells, *lists)

    def push(peer, source, target, sent, arrived):
        pltpu.make_async_remote_copy(
            src_ref=source,
            dst_ref=target,
            send_sem=sent,
            recv_sem=arrived,
            device_id=place(peer),
            device_id_type=pl.DeviceIdType.MESH,
        ).start()

    def await_all(most, sem):
        pltpu.make_async_copy(most, most, sem).wait()

    others = pl.ds(0, DEV - 1)

    def plane_body(plane, carry):
        density_of(plane, *lists, total_ref)

        @pl.when(plane == 0)
        def _():
            for load in loads[:6]:
                load.wait()
            pl.semaphore_wait(barrier, DEV - 1)

        folds = along_y(total_ref[...], y_high, y_low)
        send1[plane, :, 0] = along_x(folds[0], even_high, even_low)
        send1[plane, :, 1] = along_x(folds[1], odd_high, odd_low)
        each_peer(
            me,
            lambda peer: push(
                peer, send1.at[plane, peer], arrive1.at[me, plane], send_sem.at[0], arrive1_sem.at[plane]
            ),
        )
        arrive1[me, plane] = send1[plane, me]
        return carry

    lax.fori_loop(0, SLAB - 1, plane_body, 0)
    last = SLAB - 1
    density_of(last, *lists, total_ref)
    folds = along_y(total_ref[...], y_high, y_low)
    for q, tables in enumerate(((even_high, even_low), (odd_high, odd_low))):
        send1[last, :, q] = along_x(folds[q], *tables)
        each_peer(
            me,
            lambda peer: push(
                peer,
                send1.at[last, peer, q],
                arrive1.at[me, last, q],
                send_sem.at[0],
                arrive1_sem.at[last + q],
            ),
        )
        arrive1[me, last, q] = send1[last, me, q]

    transposed[0] = even_high[...].T
    transposed[1] = odd_high[...].T
    for load in loads[6:]:
        load.wait()
    for plane in range(last):
        await_all(arrive1.at[others, plane], arrive1_sem.at[plane])

    await_all(arrive1.at[others, last, 0], arrive1_sem.at[last])
    mix(0, green, shuffle, arrive1, send2, x_ref)
    each_peer(
        me,
        lambda peer: push(
            peer, send2.at[0, peer], arrive2.at[0, me], send_sem.at[1], arrive2_sem.at[SLAB]
        ),
    )
    arrive2[0, me] = send2[0, me]
    await_all(arrive1.at[others, last, 1], arrive1_sem.at[last + 1])
    mix(1, green, shuffle, arrive1, send2, x_ref)
    for plane in range(SLAB):
        each_peer(
            me,
            lambda peer: push(
                peer,
                send2.at[1, peer, plane],
                arrive2.at[1, me, plane],
                send_sem.at[1],
                arrive2_sem.at[plane],
            ),
        )
    arrive2[1, me] = send2[1, me]

    await_all(arrive2.at[0, others], arrive2_sem.at[SLAB])
    for plane in range(SLAB):
        halfway[plane] = back_along_x(0, plane, arrive2, unzip, transposed, turned)
    writes = [
        pltpu.make_async_copy(stage.at[plane], out.at[plane], out_sem.at[plane])
        for plane in range(SLAB)
    ]
    for plane in range(SLAB):
        await_all(arrive2.at[1, others, plane], arrive2_sem.at[plane])
        even = halfway[plane]
        odd = back_along_x(1, plane, arrive2, unzip, transposed, turned)
        middle = jnp.concatenate([even + odd, even - odd], axis=0).astype(BF16)
        stage[plane] = dot_nt(middle, y_high[...]) * (1.0 / 512.0)
        writes[plane].start()

    await_all(arrive1.at[others], send_sem.at[0])
    await_all(send2.at[:, others], send_sem.at[1])
    for write in writes:
        write.wait()


def tiles_side_by_side(tiles):
    return jnp.concatenate([tiles[:16].reshape(256, 128), tiles[16:].reshape(256, 128)], axis=1)


def mix(q, green, shuffle, arrived, out, x_ref):
    first = lax.broadcasted_iota(jnp.int32, (NZ, 128), 1) == 0

    def turn(g, carry):
        tiles = arrived[pl.ds(g * 32, 32), :, q].reshape(96, 16, 128)
        for j in range(3):
            block = tiles_side_by_side(tiles[32 * j : 32 * j + 32])
            rows = dot(shuffle[...], block).astype(BF16).reshape(16, 16, 256)
            for k in range(2):
                at = pl.ds(pl.multiple_of(g * 96 + j * 32 + k * 16, 16), 16)
                for h in range(2):
                    x_ref[q, :, at, 128 * h : 128 * h + 128] = rows[
                        8 * h : 8 * h + 8, :, 128 * k : 128 * k + 128
                    ]
        return carry

    lax.fori_loop(0, DEV // 32, turn, 0, unroll=4)

    def one_wave(r):
        rows = [r, r + 2, r + 4, r + 6]
        pr, pi, mr, mi = (x_ref[q, row] for row in rows)
        p0 = [pr[:, :128].astype(F32), pi[:, :128].astype(F32)]
        m0 = [mr[:, :128].astype(F32), mi[:, :128].astype(F32)]
        m1 = [mr[:, 128:].astype(F32), mi[:, 128:].astype(F32)]
        zero = [(p0[0] + m0[0]) * 0.5, (p0[1] + m0[1]) * 0.5]
        last = [(p0[1] - m0[1]) * 0.5, (m0[0] - p0[0]) * 0.5]
        pick = lambda a, b: jnp.concatenate(
            [jnp.where(first, x, y) for x, y in zip(a, b)], axis=1
        ).astype(BF16)
        block0 = pick(zero, p0)
        block1 = jnp.concatenate([pr[:, 128:], pi[:, 128:]], axis=1)
        block2 = pick(last, m1)
        block3 = pick(m1, m0)
        u = 2 * r + q
        y0, y1, y2, y3 = (
            dot(green[u, b], block) for b, block in enumerate((block0, block1, block2, block3))
        )
        re = lambda a: a[:, :128]
        im = lambda a: a[:, 128:]
        ar = jnp.where(first, (re(y0) - im(y2)) * 0.5, re(y0))
        ai = jnp.where(first, (im(y0) + re(y2)) * 0.5, im(y0))
        br = jnp.where(first, (re(y0) + im(y2)) * 0.5, re(y3))
        bi = jnp.where(first, (im(y0) - re(y2)) * 0.5, im(y3))
        cr = jnp.where(first, re(y3), re(y2))
        ci = jnp.where(first, im(y3), im(y2))
        x_ref[q, rows[0]] = jnp.concatenate([ar, re(y1)], axis=1).astype(BF16)
        x_ref[q, rows[1]] = jnp.concatenate([ai, im(y1)], axis=1).astype(BF16)
        x_ref[q, rows[2]] = jnp.concatenate([br, cr], axis=1).astype(BF16)
        x_ref[q, rows[3]] = jnp.concatenate([bi, ci], axis=1).astype(BF16)

    for r in range(2):
        one_wave(r)

    def turn_back(g, carry):
        tiles = []
        for j in range(3):
            pair = []
            for k in range(2):
                at = pl.ds(pl.multiple_of(g * 96 + j * 32 + k * 16, 16), 16)
                pair += [x_ref[q, :, at, :128], x_ref[q, :, at, 128:]]
            block = tiles_side_by_side(jnp.concatenate(pair, axis=0))
            rows = dot(shuffle[...], block).astype(BF16)
            tiles += [rows[:, :128].reshape(16, 16, 128), rows[:, 128:].reshape(16, 16, 128)]
        out[q, pl.ds(g * 32, 32)] = jnp.concatenate(tiles, axis=0).reshape(32, SLAB, 16, 128)
        return carry

    lax.fori_loop(0, DEV // 32, turn_back, 0, unroll=4)


def back_along_x(q, plane, arrived, unzip, transposed, turned):
    for g in range(DEV // 32):
        block = tiles_side_by_side(arrived[q, pl.ds(g * 32, 32), plane])
        rows = dot(unzip[...], block).astype(BF16)
        for k in range(2):
            for h in range(2):
                turned[q, g * 256 + k * 128 : g * 256 + k * 128 + 128, 128 * h : 128 * h + 128] = (
                    rows[128 * h : 128 * h + 128, 128 * k : 128 * k + 128]
                )
    out = dot(transposed[q], turned[q])
    return jnp.concatenate([out[:HALF], out[HALF:]], axis=1)


VMEM = pl.BlockSpec(memory_space=pltpu.VMEM)
ANY = pl.BlockSpec(memory_space=pl.ANY)


def shards(charges, cells, splines, counts, green):
    constants = [*make_tables(), make_shuffle(), make_unzip()]
    return pl.pallas_call(
        fused_kernel,
        out_shape=jax.ShapeDtypeStruct((SLAB, NX, NY), F32),
        in_specs=[pl.BlockSpec(memory_space=pltpu.SMEM)] + [VMEM] * 3 + [ANY] * 9,
        out_specs=ANY,
        scratch_shapes=[
            pltpu.VMEM((SPREAD, SLOTS), F32),
            pltpu.VMEM((SPREAD, SLOTS), F32),
            pltpu.VMEM((SPREAD, SLOTS), jnp.int32),
            pltpu.VMEM((SPREAD, SLOTS), jnp.int32),
            pltpu.VMEM((NX, NY), F32),
            *[pltpu.VMEM(table.shape, BF16) for table in constants],
            pltpu.VMEM(green.shape, BF16),
            pltpu.VMEM((SLAB, DEV, 2, 16, 128), BF16),
            pltpu.VMEM((DEV, SLAB, 2, 16, 128), BF16),
            pltpu.VMEM((2, 8, NZ, 256), BF16),
            pltpu.VMEM((2, DEV, SLAB, 16, 128), BF16),
            pltpu.VMEM((2, DEV, SLAB, 16, 128), BF16),
            pltpu.VMEM((2, DEV * 8, HALF), BF16),
            pltpu.VMEM((2, NX, DEV * 8), BF16),
            pltpu.VMEM((SLAB, HALF, NY), F32),
            pltpu.VMEM((SLAB, NX, NY), F32),
            pltpu.SemaphoreType.DMA((9,)),
            pltpu.SemaphoreType.DMA((2,)),
            pltpu.SemaphoreType.DMA((SLAB + 1,)),
            pltpu.SemaphoreType.DMA((SLAB + 1,)),
            pltpu.SemaphoreType.DMA((SLAB,)),
        ],
        compiler_params=pltpu.CompilerParams(
            collective_id=0, has_side_effects=True, vmem_limit_bytes=62 * 2**20
        ),
        name="fused",
    )(counts, charges.reshape(1, SLOTS), splines, cells, *constants, green)


def solution(mesh):
    in_specs = (
        P(("zg", "xy")),
        P(None, ("zg", "xy")),
        P(None, ("zg", "xy")),
        P(("zg", "xy")),
        P(("zg", "xy"), None, None, None),
    )
    out_specs = P(("zg", "xy"), None, None)
    return jax.shard_map(shards, mesh=mesh, in_specs=in_specs, out_specs=out_specs, check_vma=False)
```

```python
import functools
import math

import numpy as np
import jax
import jax.numpy as jnp
from jax import lax
from jax.experimental import pallas as pl
from jax.experimental.pallas import tpu as pltpu
from jax.sharding import PartitionSpec as P

NX = 512
NY = 512
NZ = 384
HALF = 256
DEV = 128
SLAB = 3
SLOTS = 2048
SPREAD = 8
CHUNK = 1024
CANDIDATES = 32
SHARES = SLOTS // CHUNK + 1
F32 = jnp.float32
BF16 = jnp.bfloat16


def split_table(table):
    high = table.astype(np.float32).astype(BF16)
    low = (table - high.astype(np.float64)).astype(np.float32).astype(BF16)
    return high, low


def make_tables():
    y = np.arange(NY)[:, None]
    v = np.arange(HALF)[None, :]
    angle = 2.0 * math.pi * (y * v % NY) / NY
    along_p = np.cos(angle)
    along_q = -np.sin(angle)
    along_q[:, 0] = 1.0 - 2.0 * (np.arange(NY) % 2)
    y_high, y_low = split_table(np.concatenate([along_p, along_q], axis=1))
    x = np.arange(HALF)[None, None, :]
    result = [y_high, y_low]
    for parity in range(2):
        u = (4 * np.arange(DEV)[:, None] + 2 * np.arange(2)[None, :] + parity)[:, :, None]
        angle = 2.0 * math.pi * (u * x % NX) / NX
        c, s = np.cos(angle), np.sin(angle)
        rows = [
            np.concatenate([c, s], axis=2),
            np.concatenate([-s, c], axis=2),
            np.concatenate([c, -s], axis=2),
            np.concatenate([-s, -c], axis=2),
        ]
        table = np.stack(rows, axis=1).reshape(DEV * 8, NX)
        result += split_table(table)
    return result


def make_shuffle():
    k, w = np.meshgrid(np.arange(16), np.arange(16), indexing="ij")
    shuffle = np.zeros((256, 256), np.float32)
    shuffle[(k * 16 + w).reshape(-1), (w * 16 + k).reshape(-1)] = 1.0
    return shuffle.astype(BF16)


def dot(a, b):
    return jnp.dot(a, b, preferred_element_type=F32)


def dot_nt(a, b):
    return lax.dot_general(a, b, (((1,), (1,)), ((), ())), preferred_element_type=F32)


def dot_tn(a, b):
    return lax.dot_general(a, b, (((0,), (0,)), ((), ())), preferred_element_type=F32)


def halves(value):
    high = value.astype(BF16)
    return high, (value - high.astype(F32)).astype(BF16)


def factor(value):
    best_left = jnp.ones_like(value)
    best_right = value.astype(BF16).astype(F32)
    best_error = jnp.abs(best_right - value)
    for j in range(1, CANDIDATES):
        left = 1.0 + j * (128 // CANDIDATES) / 128.0
        right = (value * (1.0 / left)).astype(BF16).astype(F32)
        error = jnp.abs(right * left - value)
        better = error < best_error
        best_error = jnp.where(better, error, best_error)
        best_right = jnp.where(better, right, best_right)
        best_left = jnp.where(better, left, best_left)
    return best_left, best_right


def prepare(counts, charges, splines, cells, left_ref, right_ref, row_ref, col_ref):
    slot = lax.broadcasted_iota(jnp.int32, (1, SLOTS), 1)
    live = jnp.where(slot < counts[0], charges[...], 0.0)
    left, right = factor(splines[...] * live)
    left_ref[...] = left
    right_ref[...] = right
    row_ref[...] = lax.shift_right_logical(cells[...], 9)
    col_ref[...] = lax.bitwise_and(cells[...], NY - 1)


def density_of(plane, left_ref, right_ref, row_ref, col_ref, total_ref, between=None):
    total_ref[...] = jnp.zeros_like(total_ref)
    index = lax.broadcasted_iota(jnp.int32, (NX, CHUNK), 0)
    index_row = index + plane * NX

    def body(c, carry):
        if between is not None:
            between(c)
        at = pl.ds(pl.multiple_of(c * CHUNK, CHUNK), CHUNK)
        a, b = [], []
        for k in range(SPREAD):
            a.append(jnp.where(row_ref[k : k + 1, at] == index_row, left_ref[k : k + 1, at], 0.0).astype(BF16))
            b.append(jnp.where(col_ref[k : k + 1, at] == index, right_ref[k : k + 1, at], 0.0).astype(BF16))
        total_ref[...] += dot_nt(jnp.concatenate(a, axis=1), jnp.concatenate(b, axis=1))
        return carry

    lax.fori_loop(0, SLOTS // CHUNK, body, 0)


def along_y(density, y_high, y_low):
    high, low = halves(density)
    along = dot(high, y_high[...]) + dot(high, y_low[...]) + dot(low, y_high[...])
    return along[:HALF] + along[HALF:], along[:HALF] - along[HALF:]


def along_x(fold, x_high, x_low):
    stacked = jnp.concatenate([fold[:, :HALF], fold[:, HALF:]], axis=0) * (1.0 / 512.0)
    high, low = halves(stacked)
    out = dot(x_high[...], high) + dot(x_high[...], low) + dot(x_low[...], high)
    out = out.reshape(DEV, 8, HALF)
    return jnp.concatenate([out[:, :, :128], out[:, :, 128:]], axis=1).astype(BF16)


def make_unzip():
    q, d, k = np.meshgrid(np.arange(2), np.arange(16), np.arange(8), indexing="ij")
    unzip = np.zeros((256, 256), np.float32)
    unzip[(q * 128 + d * 8 + k).reshape(-1), (d * 16 + q * 8 + k).reshape(-1)] = 1.0
    return unzip.astype(BF16)


def far_first():
    offsets = [o for o in np.ndindex(4, 4, 4, 2) if any(o)]
    hops = lambda o: sum(min(d, 4 - d) for d in o[:3])
    return sorted(offsets, key=lambda o: (-hops(o), o))


def each_peer(action, share=0, shares=1):
    low = lax.axis_index("zg")
    index = lax.axis_index("xy")
    along = 2 * (index // 32) + low
    x = [lax.rem(along + d, 4) for d in range(4)]
    x_low = [lax.rem(a, 2) for a in x]
    x_high = [32 * (a // 2) for a in x]
    y = [8 * lax.rem(lax.rem(index // 8, 4) + d, 4) for d in range(4)]
    z = [2 * lax.rem(lax.rem(index // 2, 4) + d, 4) for d in range(4)]
    core = [lax.rem(index + d, 2) for d in range(2)]
    order = far_first()
    each = -(-len(order) // shares)
    for dx, dy, dz, dc in order[each * share : each * (share + 1)]:
        inner = x_high[dx] + y[dy] + z[dz] + core[dc]
        action(64 * x_low[dx] + inner, (x_low[dx], inner))


def fused_kernel(counts, charges, splines, cells, *rest):
    sources, out, middle_out = rest[:9], rest[9], rest[10]
    lists, total_ref = rest[11:15], rest[15]
    held = rest[16:25]
    send1, arrive1, x_ref, send2, arrive2, turned, transposed, halfway, stage, middle = rest[25:35]
    load_sem, send_sem, arrive1_sem, arrive2_sem, out_sem = rest[35:40]
    y_high, y_low, even_high, even_low, odd_high, odd_low, shuffle, unzip, green = held
    me = lax.axis_index("zg") * 64 + lax.axis_index("xy")
    barrier = pltpu.get_barrier_semaphore()

    loads = [
        pltpu.make_async_copy(source, target, load_sem.at[i])
        for i, (source, target) in enumerate(zip(sources, held))
    ]
    for load in loads:
        load.start()

    def greet(peer, place):
        pl.semaphore_signal(
            barrier, inc=1, device_id=place, device_id_type=pl.DeviceIdType.MESH
        )

    each_peer(greet)
    prepare(counts, charges, splines, cells, *lists)

    def push(place, source, target, sent, arrived):
        pltpu.make_async_remote_copy(
            src_ref=source,
            dst_ref=target,
            send_sem=sent,
            recv_sem=arrived,
            device_id=place,
            device_id_type=pl.DeviceIdType.MESH,
        ).start()

    def await_all(most, sem):
        pltpu.make_async_copy(most, most, sem).wait()

    others = pl.ds(0, DEV - 1)

    def send_plane(plane, share, shares):
        each_peer(
            lambda peer, place: push(
                place, send1.at[plane, peer], arrive1.at[me, plane], send_sem.at[0], arrive1_sem.at[plane]
            ),
            share,
            shares,
        )

    def send_between(plane):
        def between(c):
            for share in range(SLOTS // CHUNK):

                @pl.when(c == share)
                def _():
                    send_plane(plane, share, SHARES)

        return between

    last = SLAB - 1
    for plane in range(SLAB):
        density_of(plane, *lists, total_ref, send_between(plane - 1) if plane else None)
        if plane > 0:
            send_plane(plane - 1, SHARES - 1, SHARES)
        if plane == 0:
            for load in loads[:6]:
                load.wait()
            pl.semaphore_wait(barrier, DEV - 1)
        if plane < last:
            folds = along_y(total_ref[...], y_high, y_low)
            send1[plane, :, 0] = along_x(folds[0], even_high, even_low)
            send1[plane, :, 1] = along_x(folds[1], odd_high, odd_low)
            arrive1[me, plane] = send1[plane, me]
    folds = along_y(total_ref[...], y_high, y_low)
    for q, tables in enumerate(((even_high, even_low), (odd_high, odd_low))):
        send1[last, :, q] = along_x(folds[q], *tables)
        each_peer(
            lambda peer, place: push(
                place,
                send1.at[last, peer, q],
                arrive1.at[me, last, q],
                send_sem.at[0],
                arrive1_sem.at[last + q],
            ),
        )
        arrive1[me, last, q] = send1[last, me, q]

    transposed[0] = even_high[...].T
    transposed[1] = odd_high[...].T
    for load in loads[6:]:
        load.wait()
    for plane in range(last):
        await_all(arrive1.at[others, plane], arrive1_sem.at[plane])

    await_all(arrive1.at[others, last, 0], arrive1_sem.at[last])
    mix(0, green, shuffle, arrive1, send2, x_ref)
    each_peer(
        lambda peer, place: push(
            place, send2.at[0, peer], arrive2.at[0, me], send_sem.at[1], arrive2_sem.at[SLAB]
        ),
    )
    arrive2[0, me] = send2[0, me]
    await_all(arrive1.at[others, last, 1], arrive1_sem.at[last + 1])
    mix(1, green, shuffle, arrive1, send2, x_ref)
    for plane in range(SLAB):
        each_peer(
            lambda peer, place: push(
                place,
                send2.at[1, peer, plane],
                arrive2.at[1, me, plane],
                send_sem.at[1],
                arrive2_sem.at[plane],
            ),
        )
    arrive2[1, me] = send2[1, me]

    await_all(arrive2.at[0, others], arrive2_sem.at[SLAB])
    for plane in range(SLAB):
        halfway[plane] = back_along_x(0, plane, arrive2, unzip, transposed, turned)
    writes = [
        pltpu.make_async_copy(stage.at[plane], out.at[plane], out_sem.at[plane])
        for plane in range(last)
    ] + [pltpu.make_async_copy(middle, middle_out, out_sem.at[last])]
    for plane in range(SLAB):
        await_all(arrive2.at[1, others, plane], arrive2_sem.at[plane])
        even = halfway[plane]
        odd = back_along_x(1, plane, arrive2, unzip, transposed, turned)
        value = jnp.concatenate([even + odd, even - odd], axis=0).astype(BF16)
        if plane < last:
            stage[plane] = dot_nt(value, y_high[...]) * (1.0 / 512.0)
        else:
            middle[...] = value
        writes[plane].start()

    await_all(arrive1.at[others], send_sem.at[0])
    await_all(send2.at[:, others], send_sem.at[1])
    for write in writes:
        write.wait()


def tiles_side_by_side(tiles):
    return jnp.concatenate([tiles[:16].reshape(256, 128), tiles[16:].reshape(256, 128)], axis=1)


def mix(q, green, shuffle, arrived, out, x_ref):
    first = lax.broadcasted_iota(jnp.int32, (NZ, 128), 1) == 0

    def turn(g, carry):
        tiles = arrived[pl.ds(g * 32, 32), :, q].reshape(96, 16, 128)
        for j in range(3):
            block = tiles_side_by_side(tiles[32 * j : 32 * j + 32])
            rows = dot(shuffle[...], block).astype(BF16).reshape(16, 16, 256)
            for k in range(2):
                at = pl.ds(pl.multiple_of(g * 96 + j * 32 + k * 16, 16), 16)
                for h in range(2):
                    x_ref[q, :, at, 128 * h : 128 * h + 128] = rows[
                        8 * h : 8 * h + 8, :, 128 * k : 128 * k + 128
                    ]
        return carry

    lax.fori_loop(0, DEV // 32, turn, 0, unroll=4)

    def one_wave(r):
        rows = [r, r + 2, r + 4, r + 6]
        pr, pi, mr, mi = (x_ref[q, row] for row in rows)
        p0 = [pr[:, :128].astype(F32), pi[:, :128].astype(F32)]
        m0 = [mr[:, :128].astype(F32), mi[:, :128].astype(F32)]
        m1 = [mr[:, 128:].astype(F32), mi[:, 128:].astype(F32)]
        zero = [(p0[0] + m0[0]) * 0.5, (p0[1] + m0[1]) * 0.5]
        last = [(p0[1] - m0[1]) * 0.5, (m0[0] - p0[0]) * 0.5]
        pick = lambda a, b: jnp.concatenate(
            [jnp.where(first, x, y) for x, y in zip(a, b)], axis=1
        ).astype(BF16)
        block0 = pick(zero, p0)
        block1 = jnp.concatenate([pr[:, 128:], pi[:, 128:]], axis=1)
        block2 = pick(last, m1)
        block3 = pick(m1, m0)
        u = 2 * r + q
        y0, y1, y2, y3 = (
            dot(green[u, b], block) for b, block in enumerate((block0, block1, block2, block3))
        )
        re = lambda a: a[:, :128]
        im = lambda a: a[:, 128:]
        ar = jnp.where(first, (re(y0) - im(y2)) * 0.5, re(y0))
        ai = jnp.where(first, (im(y0) + re(y2)) * 0.5, im(y0))
        br = jnp.where(first, (re(y0) + im(y2)) * 0.5, re(y3))
        bi = jnp.where(first, (im(y0) - re(y2)) * 0.5, im(y3))
        cr = jnp.where(first, re(y3), re(y2))
        ci = jnp.where(first, im(y3), im(y2))
        x_ref[q, rows[0]] = jnp.concatenate([ar, re(y1)], axis=1).astype(BF16)
        x_ref[q, rows[1]] = jnp.concatenate([ai, im(y1)], axis=1).astype(BF16)
        x_ref[q, rows[2]] = jnp.concatenate([br, cr], axis=1).astype(BF16)
        x_ref[q, rows[3]] = jnp.concatenate([bi, ci], axis=1).astype(BF16)

    for r in range(2):
        one_wave(r)

    def turn_back(g, carry):
        tiles = []
        for j in range(3):
            pair = []
            for k in range(2):
                at = pl.ds(pl.multiple_of(g * 96 + j * 32 + k * 16, 16), 16)
                pair += [x_ref[q, :, at, :128], x_ref[q, :, at, 128:]]
            block = tiles_side_by_side(jnp.concatenate(pair, axis=0))
            rows = dot(shuffle[...], block).astype(BF16)
            tiles += [rows[:, :128].reshape(16, 16, 128), rows[:, 128:].reshape(16, 16, 128)]
        out[q, pl.ds(g * 32, 32)] = jnp.concatenate(tiles, axis=0).reshape(32, SLAB, 16, 128)
        return carry

    lax.fori_loop(0, DEV // 32, turn_back, 0, unroll=4)


def back_along_x(q, plane, arrived, unzip, transposed, turned):
    for g in range(DEV // 32):
        block = tiles_side_by_side(arrived[q, pl.ds(g * 32, 32), plane])
        rows = dot(unzip[...], block).astype(BF16)
        for k in range(2):
            for h in range(2):
                turned[q, g * 256 + k * 128 : g * 256 + k * 128 + 128, 128 * h : 128 * h + 128] = (
                    rows[128 * h : 128 * h + 128, 128 * k : 128 * k + 128]
                )
    out = dot(transposed[q], turned[q])
    return jnp.concatenate([out[:HALF], out[HALF:]], axis=1)


def finish_kernel(part, middle, y_high, out, middle_ref, y_ref, stage, load_sem, write_sem):
    last = SLAB - 1
    loads = [
        pltpu.make_async_copy(source, target, load_sem.at[i])
        for i, (source, target) in enumerate(
            ((part.at[0], stage.at[0]), (part.at[1], stage.at[1]), (middle, middle_ref), (y_high, y_ref))
        )
    ]
    writes = [
        pltpu.make_async_copy(stage.at[plane], out.at[plane], write_sem.at[plane])
        for plane in range(SLAB)
    ]
    for load in loads:
        load.start()
    for plane in range(last):
        loads[plane].wait()
        writes[plane].start()
    loads[2].wait()
    loads[3].wait()
    stage[last] = dot_nt(middle_ref[...], y_ref[...]) * (1.0 / 512.0)
    writes[last].start()
    for write in writes:
        write.wait()


VMEM = pl.BlockSpec(memory_space=pltpu.VMEM)
ANY = pl.BlockSpec(memory_space=pl.ANY)


def shards(charges, cells, splines, counts, green):
    constants = [*make_tables(), make_shuffle(), make_unzip()]
    part, middle = pl.pallas_call(
        fused_kernel,
        out_shape=(
            jax.ShapeDtypeStruct((SLAB - 1, NX, NY), F32),
            jax.ShapeDtypeStruct((NX, NY), BF16),
        ),
        in_specs=[pl.BlockSpec(memory_space=pltpu.SMEM)] + [VMEM] * 3 + [ANY] * 9,
        out_specs=(ANY, ANY),
        scratch_shapes=[
            pltpu.VMEM((SPREAD, SLOTS), F32),
            pltpu.VMEM((SPREAD, SLOTS), F32),
            pltpu.VMEM((SPREAD, SLOTS), jnp.int32),
            pltpu.VMEM((SPREAD, SLOTS), jnp.int32),
            pltpu.VMEM((NX, NY), F32),
            *[pltpu.VMEM(table.shape, BF16) for table in constants],
            pltpu.VMEM(green.shape, BF16),
            pltpu.VMEM((SLAB, DEV, 2, 16, 128), BF16),
            pltpu.VMEM((DEV, SLAB, 2, 16, 128), BF16),
            pltpu.VMEM((2, 8, NZ, 256), BF16),
            pltpu.VMEM((2, DEV, SLAB, 16, 128), BF16),
            pltpu.VMEM((2, DEV, SLAB, 16, 128), BF16),
            pltpu.VMEM((2, DEV * 8, HALF), BF16),
            pltpu.VMEM((2, NX, DEV * 8), BF16),
            pltpu.VMEM((SLAB, HALF, NY), F32),
            pltpu.VMEM((SLAB - 1, NX, NY), F32),
            pltpu.VMEM((NX, NY), BF16),
            pltpu.SemaphoreType.DMA((9,)),
            pltpu.SemaphoreType.DMA((2,)),
            pltpu.SemaphoreType.DMA((SLAB + 1,)),
            pltpu.SemaphoreType.DMA((SLAB + 1,)),
            pltpu.SemaphoreType.DMA((SLAB,)),
        ],
        compiler_params=pltpu.CompilerParams(
            collective_id=0, has_side_effects=True, vmem_limit_bytes=62 * 2**20
        ),
        name="fused",
    )(counts, charges.reshape(1, SLOTS), splines, cells, *constants, green)
    return pl.pallas_call(
        finish_kernel,
        out_shape=jax.ShapeDtypeStruct((SLAB, NX, NY), F32),
        in_specs=[ANY] * 3,
        out_specs=ANY,
        scratch_shapes=[
            pltpu.VMEM((NX, NY), BF16),
            pltpu.VMEM((NY, NY), BF16),
            pltpu.VMEM((SLAB, NX, NY), F32),
            pltpu.SemaphoreType.DMA((4,)),
            pltpu.SemaphoreType.DMA((SLAB,)),
        ],
        name="finish",
    )(part, middle, constants[0])


def solution(mesh):
    in_specs = (
        P(("zg", "xy")),
        P(None, ("zg", "xy")),
        P(None, ("zg", "xy")),
        P(("zg", "xy")),
        P(("zg", "xy"), None, None, None),
    )
    out_specs = P(("zg", "xy"), None, None)
    return jax.shard_map(shards, mesh=mesh, in_specs=in_specs, out_specs=out_specs, check_vma=False)
```

```python
import functools
import math

import numpy as np
import jax
import jax.numpy as jnp
from jax import lax
from jax.experimental import pallas as pl
from jax.experimental.pallas import tpu as pltpu
from jax.sharding import PartitionSpec as P

NX = 512
NY = 512
NZ = 384
HALF = 256
DEV = 128
SLAB = 3
SLOTS = 2048
SPREAD = 8
CHUNK = 1024
CANDIDATES = 16
SHARES = SLOTS // CHUNK + 1
F32 = jnp.float32
BF16 = jnp.bfloat16


def split_table(table):
    high = table.astype(np.float32).astype(BF16)
    low = (table - high.astype(np.float64)).astype(np.float32).astype(BF16)
    return high, low


def make_tables():
    y = np.arange(NY)[:, None]
    v = np.arange(HALF)[None, :]
    angle = 2.0 * math.pi * (y * v % NY) / NY
    along_p = np.cos(angle)
    along_q = -np.sin(angle)
    along_q[:, 0] = 1.0 - 2.0 * (np.arange(NY) % 2)
    y_high, y_low = split_table(np.concatenate([along_p, along_q], axis=1))
    x = np.arange(HALF)[None, None, :]
    result = [y_high, y_low]
    for parity in range(2):
        u = (4 * np.arange(DEV)[:, None] + 2 * np.arange(2)[None, :] + parity)[:, :, None]
        angle = 2.0 * math.pi * (u * x % NX) / NX
        c, s = np.cos(angle), np.sin(angle)
        rows = [
            np.concatenate([c, s], axis=2),
            np.concatenate([-s, c], axis=2),
            np.concatenate([c, -s], axis=2),
            np.concatenate([-s, -c], axis=2),
        ]
        table = np.stack(rows, axis=1).reshape(DEV * 8, NX)
        result += split_table(table)
    return result


def make_shuffle():
    k, w = np.meshgrid(np.arange(16), np.arange(16), indexing="ij")
    shuffle = np.zeros((256, 256), np.float32)
    shuffle[(k * 16 + w).reshape(-1), (w * 16 + k).reshape(-1)] = 1.0
    return shuffle.astype(BF16)


def dot(a, b):
    return jnp.dot(a, b, preferred_element_type=F32)


def dot_nt(a, b):
    return lax.dot_general(a, b, (((1,), (1,)), ((), ())), preferred_element_type=F32)


def dot_tn(a, b):
    return lax.dot_general(a, b, (((0,), (0,)), ((), ())), preferred_element_type=F32)


def halves(value):
    high = value.astype(BF16)
    return high, (value - high.astype(F32)).astype(BF16)


def factor(value):
    best_left = jnp.ones_like(value)
    best_right = value.astype(BF16).astype(F32)
    best_error = jnp.abs(best_right - value)
    for j in range(1, CANDIDATES):
        left = 1.0 + j * (128 // CANDIDATES) / 128.0
        right = (value * (1.0 / left)).astype(BF16).astype(F32)
        error = jnp.abs(right * left - value)
        better = error < best_error
        best_error = jnp.where(better, error, best_error)
        best_right = jnp.where(better, right, best_right)
        best_left = jnp.where(better, left, best_left)
    return best_left, best_right


def prepare(counts, charges, splines, cells, left_ref, right_ref, row_ref, col_ref):
    slot = lax.broadcasted_iota(jnp.int32, (1, SLOTS), 1)
    live = jnp.where(slot < counts[0], charges[...], 0.0)
    left, right = factor(splines[...] * live)
    left_ref[...] = left
    right_ref[...] = right
    row_ref[...] = lax.shift_right_logical(cells[...], 9)
    col_ref[...] = lax.bitwise_and(cells[...], NY - 1)


def density_of(plane, left_ref, right_ref, row_ref, col_ref, between=None):
    index = lax.broadcasted_iota(jnp.int32, (NX, CHUNK), 0)
    index_row = index + plane * NX
    total = None
    for c in range(SLOTS // CHUNK):
        if between is not None:
            between(c)
        at = slice(c * CHUNK, c * CHUNK + CHUNK)
        a, b = [], []
        for k in range(SPREAD):
            a.append(jnp.where(row_ref[k : k + 1, at] == index_row, left_ref[k : k + 1, at], 0.0).astype(BF16))
            b.append(jnp.where(col_ref[k : k + 1, at] == index, right_ref[k : k + 1, at], 0.0).astype(BF16))
        part = dot_nt(jnp.concatenate(a, axis=1), jnp.concatenate(b, axis=1))
        total = part if total is None else total + part
    return total


def along_y(density, y_high, y_low):
    high, low = halves(density)
    along = dot(high, y_high[...]) + dot(high, y_low[...]) + dot(low, y_high[...])
    return along[:HALF] + along[HALF:], along[:HALF] - along[HALF:]


def along_x(fold, x_high, x_low):
    stacked = jnp.concatenate([fold[:, :HALF], fold[:, HALF:]], axis=0) * (1.0 / 512.0)
    high, low = halves(stacked)
    out = dot(x_high[...], high) + dot(x_high[...], low) + dot(x_low[...], high)
    out = out.reshape(DEV, 8, HALF)
    return jnp.concatenate([out[:, :, :128], out[:, :, 128:]], axis=1).astype(BF16)


def make_unzip():
    q, d, k = np.meshgrid(np.arange(2), np.arange(16), np.arange(8), indexing="ij")
    unzip = np.zeros((256, 256), np.float32)
    unzip[(q * 128 + d * 8 + k).reshape(-1), (d * 16 + q * 8 + k).reshape(-1)] = 1.0
    return unzip.astype(BF16)


def far_first():
    offsets = [o for o in np.ndindex(4, 4, 4, 2) if any(o)]
    hops = lambda o: sum(min(d, 4 - d) for d in o[:3])
    return sorted(offsets, key=lambda o: (-hops(o), o))


def each_peer(action, share=0, shares=1):
    low = lax.axis_index("zg")
    index = lax.axis_index("xy")
    along = 2 * (index // 32) + low
    x = [lax.rem(along + d, 4) for d in range(4)]
    x_low = [lax.rem(a, 2) for a in x]
    x_high = [32 * (a // 2) for a in x]
    y = [8 * lax.rem(lax.rem(index // 8, 4) + d, 4) for d in range(4)]
    z = [2 * lax.rem(lax.rem(index // 2, 4) + d, 4) for d in range(4)]
    core = [lax.rem(index + d, 2) for d in range(2)]
    order = far_first()
    each = -(-len(order) // shares)
    for dx, dy, dz, dc in order[each * share : each * (share + 1)]:
        inner = x_high[dx] + y[dy] + z[dz] + core[dc]
        action(64 * x_low[dx] + inner, (x_low[dx], inner))


def fused_kernel(counts, charges, splines, cells, *rest):
    sources, out, middle_out = rest[:9], rest[9], rest[10]
    lists, total_ref = rest[11:15], rest[15]
    held = rest[16:25]
    send1, arrive1, x_ref, send2, arrive2, turned, transposed, halfway, stage, middle = rest[25:35]
    load_sem, send_sem, arrive1_sem, arrive2_sem, out_sem = rest[35:40]
    y_high, y_low, even_high, even_low, odd_high, odd_low, shuffle, unzip, green = held
    me = lax.axis_index("zg") * 64 + lax.axis_index("xy")
    barrier = pltpu.get_barrier_semaphore()

    loads = [
        pltpu.make_async_copy(source, target, load_sem.at[i])
        for i, (source, target) in enumerate(zip(sources, held))
    ]
    for load in loads:
        load.start()

    def greet(peer, place):
        pl.semaphore_signal(
            barrier, inc=1, device_id=place, device_id_type=pl.DeviceIdType.MESH
        )

    each_peer(greet)
    prepare(counts, charges, splines, cells, *lists)

    def push(place, source, target, sent, arrived):
        pltpu.make_async_remote_copy(
            src_ref=source,
            dst_ref=target,
            send_sem=sent,
            recv_sem=arrived,
            device_id=place,
            device_id_type=pl.DeviceIdType.MESH,
        ).start()

    def await_all(most, sem):
        pltpu.make_async_copy(most, most, sem).wait()

    others = pl.ds(0, DEV - 1)

    def send_plane(plane, share, shares):
        each_peer(
            lambda peer, place: push(
                place, send1.at[plane, peer], arrive1.at[me, plane], send_sem.at[0], arrive1_sem.at[plane]
            ),
            share,
            shares,
        )

    def send_between(plane):
        return lambda c: send_plane(plane, c, SHARES)

    last = SLAB - 1
    for plane in range(SLAB):
        density = density_of(plane, *lists, send_between(plane - 1) if plane else None)
        total_ref[...] = density
        if plane > 0:
            send_plane(plane - 1, SHARES - 1, SHARES)
        if plane == 0:
            for load in loads[:6]:
                load.wait()
            pl.semaphore_wait(barrier, DEV - 1)
        if plane < last:
            folds = along_y(total_ref[...], y_high, y_low)
            send1[plane, :, 0] = along_x(folds[0], even_high, even_low)
            send1[plane, :, 1] = along_x(folds[1], odd_high, odd_low)
            arrive1[me, plane] = send1[plane, me]
    folds = along_y(total_ref[...], y_high, y_low)
    for q, tables in enumerate(((even_high, even_low), (odd_high, odd_low))):
        send1[last, :, q] = along_x(folds[q], *tables)
        each_peer(
            lambda peer, place: push(
                place,
                send1.at[last, peer, q],
                arrive1.at[me, last, q],
                send_sem.at[0],
                arrive1_sem.at[last + q],
            ),
        )
        arrive1[me, last, q] = send1[last, me, q]

    transposed[0] = even_high[...].T
    transposed[1] = odd_high[...].T
    for load in loads[6:]:
        load.wait()
    for plane in range(last):
        await_all(arrive1.at[others, plane], arrive1_sem.at[plane])

    await_all(arrive1.at[others, last, 0], arrive1_sem.at[last])
    mix(0, green, shuffle, arrive1, send2, x_ref)
    each_peer(
        lambda peer, place: push(
            place, send2.at[0, peer], arrive2.at[0, me], send_sem.at[1], arrive2_sem.at[SLAB]
        ),
    )
    arrive2[0, me] = send2[0, me]
    await_all(arrive1.at[others, last, 1], arrive1_sem.at[last + 1])
    mix(1, green, shuffle, arrive1, send2, x_ref)
    for plane in range(SLAB):
        each_peer(
            lambda peer, place: push(
                place,
                send2.at[1, peer, plane],
                arrive2.at[1, me, plane],
                send_sem.at[1],
                arrive2_sem.at[plane],
            ),
        )
    arrive2[1, me] = send2[1, me]

    await_all(arrive2.at[0, others], arrive2_sem.at[SLAB])
    for plane in range(SLAB):
        halfway[plane] = back_along_x(0, plane, arrive2, unzip, transposed, turned)
    writes = [
        pltpu.make_async_copy(stage.at[plane], out.at[plane], out_sem.at[plane])
        for plane in range(last)
    ] + [pltpu.make_async_copy(middle, middle_out, out_sem.at[last])]
    for plane in range(SLAB):
        await_all(arrive2.at[1, others, plane], arrive2_sem.at[plane])
        even = halfway[plane]
        odd = back_along_x(1, plane, arrive2, unzip, transposed, turned)
        value = jnp.concatenate([even + odd, even - odd], axis=0).astype(BF16)
        if plane < last:
            stage[plane] = dot_nt(value, y_high[...]) * (1.0 / 512.0)
        else:
            middle[...] = value
        writes[plane].start()

    await_all(arrive1.at[others], send_sem.at[0])
    await_all(send2.at[:, others], send_sem.at[1])
    for write in writes:
        write.wait()


def tiles_side_by_side(tiles):
    return jnp.concatenate([tiles[:16].reshape(256, 128), tiles[16:].reshape(256, 128)], axis=1)


def mix(q, green, shuffle, arrived, out, x_ref):
    first = lax.broadcasted_iota(jnp.int32, (NZ, 128), 1) == 0

    def turn(g, carry):
        tiles = arrived[pl.ds(g * 32, 32), :, q].reshape(96, 16, 128)
        for j in range(3):
            block = tiles_side_by_side(tiles[32 * j : 32 * j + 32])
            rows = dot(shuffle[...], block).astype(BF16).reshape(16, 16, 256)
            for k in range(2):
                at = pl.ds(pl.multiple_of(g * 96 + j * 32 + k * 16, 16), 16)
                for h in range(2):
                    x_ref[q, :, at, 128 * h : 128 * h + 128] = rows[
                        8 * h : 8 * h + 8, :, 128 * k : 128 * k + 128
                    ]
        return carry

    lax.fori_loop(0, DEV // 32, turn, 0, unroll=4)

    def one_wave(r):
        rows = [r, r + 2, r + 4, r + 6]
        pr, pi, mr, mi = (x_ref[q, row] for row in rows)
        p0 = [pr[:, :128].astype(F32), pi[:, :128].astype(F32)]
        m0 = [mr[:, :128].astype(F32), mi[:, :128].astype(F32)]
        m1 = [mr[:, 128:].astype(F32), mi[:, 128:].astype(F32)]
        zero = [(p0[0] + m0[0]) * 0.5, (p0[1] + m0[1]) * 0.5]
        last = [(p0[1] - m0[1]) * 0.5, (m0[0] - p0[0]) * 0.5]
        pick = lambda a, b: jnp.concatenate(
            [jnp.where(first, x, y) for x, y in zip(a, b)], axis=1
        ).astype(BF16)
        block0 = pick(zero, p0)
        block1 = jnp.concatenate([pr[:, 128:], pi[:, 128:]], axis=1)
        block2 = pick(last, m1)
        block3 = pick(m1, m0)
        u = 2 * r + q
        y0, y1, y2, y3 = (
            dot(green[u, b], block) for b, block in enumerate((block0, block1, block2, block3))
        )
        re = lambda a: a[:, :128]
        im = lambda a: a[:, 128:]
        ar = jnp.where(first, (re(y0) - im(y2)) * 0.5, re(y0))
        ai = jnp.where(first, (im(y0) + re(y2)) * 0.5, im(y0))
        br = jnp.where(first, (re(y0) + im(y2)) * 0.5, re(y3))
        bi = jnp.where(first, (im(y0) - re(y2)) * 0.5, im(y3))
        cr = jnp.where(first, re(y3), re(y2))
        ci = jnp.where(first, im(y3), im(y2))
        x_ref[q, rows[0]] = jnp.concatenate([ar, re(y1)], axis=1).astype(BF16)
        x_ref[q, rows[1]] = jnp.concatenate([ai, im(y1)], axis=1).astype(BF16)
        x_ref[q, rows[2]] = jnp.concatenate([br, cr], axis=1).astype(BF16)
        x_ref[q, rows[3]] = jnp.concatenate([bi, ci], axis=1).astype(BF16)

    for r in range(2):
        one_wave(r)

    def turn_back(g, carry):
        tiles = []
        for j in range(3):
            pair = []
            for k in range(2):
                at = pl.ds(pl.multiple_of(g * 96 + j * 32 + k * 16, 16), 16)
                pair += [x_ref[q, :, at, :128], x_ref[q, :, at, 128:]]
            block = tiles_side_by_side(jnp.concatenate(pair, axis=0))
            rows = dot(shuffle[...], block).astype(BF16)
            tiles += [rows[:, :128].reshape(16, 16, 128), rows[:, 128:].reshape(16, 16, 128)]
        out[q, pl.ds(g * 32, 32)] = jnp.concatenate(tiles, axis=0).reshape(32, SLAB, 16, 128)
        return carry

    lax.fori_loop(0, DEV // 32, turn_back, 0, unroll=4)


def back_along_x(q, plane, arrived, unzip, transposed, turned):
    for g in range(DEV // 32):
        block = tiles_side_by_side(arrived[q, pl.ds(g * 32, 32), plane])
        rows = dot(unzip[...], block).astype(BF16)
        for k in range(2):
            for h in range(2):
                turned[q, g * 256 + k * 128 : g * 256 + k * 128 + 128, 128 * h : 128 * h + 128] = (
                    rows[128 * h : 128 * h + 128, 128 * k : 128 * k + 128]
                )
    out = dot(transposed[q], turned[q])
    return jnp.concatenate([out[:HALF], out[HALF:]], axis=1)


def finish_kernel(part, middle, y_high, out, middle_ref, y_ref, stage, load_sem, write_sem):
    last = SLAB - 1
    loads = [
        pltpu.make_async_copy(source, target, load_sem.at[i])
        for i, (source, target) in enumerate(
            ((part.at[0], stage.at[0]), (part.at[1], stage.at[1]), (middle, middle_ref), (y_high, y_ref))
        )
    ]
    writes = [
        pltpu.make_async_copy(stage.at[plane], out.at[plane], write_sem.at[plane])
        for plane in range(SLAB)
    ]
    for load in loads:
        load.start()
    for plane in range(last):
        loads[plane].wait()
        writes[plane].start()
    loads[2].wait()
    loads[3].wait()
    stage[last] = dot_nt(middle_ref[...], y_ref[...]) * (1.0 / 512.0)
    writes[last].start()
    for write in writes:
        write.wait()


VMEM = pl.BlockSpec(memory_space=pltpu.VMEM)
ANY = pl.BlockSpec(memory_space=pl.ANY)


def shards(charges, cells, splines, counts, green):
    constants = [*make_tables(), make_shuffle(), make_unzip()]
    part, middle = pl.pallas_call(
        fused_kernel,
        out_shape=(
            jax.ShapeDtypeStruct((SLAB - 1, NX, NY), F32),
            jax.ShapeDtypeStruct((NX, NY), BF16),
        ),
        in_specs=[pl.BlockSpec(memory_space=pltpu.SMEM)] + [VMEM] * 3 + [ANY] * 9,
        out_specs=(ANY, ANY),
        scratch_shapes=[
            pltpu.VMEM((SPREAD, SLOTS), F32),
            pltpu.VMEM((SPREAD, SLOTS), F32),
            pltpu.VMEM((SPREAD, SLOTS), jnp.int32),
            pltpu.VMEM((SPREAD, SLOTS), jnp.int32),
            pltpu.VMEM((NX, NY), F32),
            *[pltpu.VMEM(table.shape, BF16) for table in constants],
            pltpu.VMEM(green.shape, BF16),
            pltpu.VMEM((SLAB, DEV, 2, 16, 128), BF16),
            pltpu.VMEM((DEV, SLAB, 2, 16, 128), BF16),
            pltpu.VMEM((2, 8, NZ, 256), BF16),
            pltpu.VMEM((2, DEV, SLAB, 16, 128), BF16),
            pltpu.VMEM((2, DEV, SLAB, 16, 128), BF16),
            pltpu.VMEM((2, DEV * 8, HALF), BF16),
            pltpu.VMEM((2, NX, DEV * 8), BF16),
            pltpu.VMEM((SLAB, HALF, NY), F32),
            pltpu.VMEM((SLAB - 1, NX, NY), F32),
            pltpu.VMEM((NX, NY), BF16),
            pltpu.SemaphoreType.DMA((9,)),
            pltpu.SemaphoreType.DMA((2,)),
            pltpu.SemaphoreType.DMA((SLAB + 1,)),
            pltpu.SemaphoreType.DMA((SLAB + 1,)),
            pltpu.SemaphoreType.DMA((SLAB,)),
        ],
        compiler_params=pltpu.CompilerParams(
            collective_id=0, has_side_effects=True, vmem_limit_bytes=62 * 2**20
        ),
        name="fused",
    )(counts, charges.reshape(1, SLOTS), splines, cells, *constants, green)
    return pl.pallas_call(
        finish_kernel,
        out_shape=jax.ShapeDtypeStruct((SLAB, NX, NY), F32),
        in_specs=[ANY] * 3,
        out_specs=ANY,
        scratch_shapes=[
            pltpu.VMEM((NX, NY), BF16),
            pltpu.VMEM((NY, NY), BF16),
            pltpu.VMEM((SLAB, NX, NY), F32),
            pltpu.SemaphoreType.DMA((4,)),
            pltpu.SemaphoreType.DMA((SLAB,)),
        ],
        name="finish",
    )(part, middle, constants[0])


def solution(mesh):
    in_specs = (
        P(("zg", "xy")),
        P(None, ("zg", "xy")),
        P(None, ("zg", "xy")),
        P(("zg", "xy")),
        P(("zg", "xy"), None, None, None),
    )
    out_specs = P(("zg", "xy"), None, None)
    return jax.shard_map(shards, mesh=mesh, in_specs=in_specs, out_specs=out_specs, check_vma=False)
```
